8 devices in a mesh: rep: 1 (over z), emb: 2 (over y), model: 4 (over x, core).
Axes of the slice: x: 2, y: 2, z: 1, core: 2. Of those that a mesh axis runs over, the one named last changes fastest.
Arguments:
- x: bfloat16 [512, 8192], P('rep')
- Wq: bfloat16 [8192, 8192], P('emb', 'model')
- Wk: bfloat16 [8192, 256], replicated
- Wv: bfloat16 [8192, 256], replicated
- Wo: bfloat16 [8192, 8192], P('model', 'emb')
- Kc: bfloat16 [512, 2048, 256], P('rep')
- Vc: bfloat16 [512, 2048, 256], P('rep')
- lengths: int32 [512], P('rep')
Outputs:
- output 1: bfloat16 [512, 8192], P('rep')
- output 2: bfloat16 [512, 256], P('rep')
- output 3: bfloat16 [512, 256], P('rep')
All inputs are finite; a program needn't handle non-finite values.
Results may differ from the reference program's by a relative error of at most 0.0108907.
Values are sent between devices in bfloat16 or wider.
A program may use at most 4.25 GiB of HBM per device.

```python
import jax
import jax.numpy as jnp
from jax import lax

B = 512
T = 2048
D = 8192
H = 32
DH = 256


def setup_inputs(seed: int = 0, part: int = 0) -> dict:
    kshared, kpart = jax.random.split(jax.random.key(seed))
    kpart = jax.random.fold_in(kpart, part)
    kq, kk, kv, ko = jax.random.split(kshared, 4)
    kx, kkc, kvc, kl = jax.random.split(kpart, 4)
    x = jax.random.normal(kx, (B, D), jnp.float32)
    Wq = jax.random.normal(kq, (D, H * DH), jnp.float32) * (2.5 * D ** -0.5)
    Wk = jax.random.normal(kk, (D, DH), jnp.float32) * D ** -0.5
    Wv = jax.random.normal(kv, (D, DH), jnp.float32) * D ** -0.5
    Wo = jax.random.normal(ko, (H * DH, D), jnp.float32) * (3.0 * (H * DH) ** -0.5)
    Kc = jax.random.normal(kkc, (B, T, DH), jnp.float32)
    Vc = jax.random.normal(kvc, (B, T, DH), jnp.float32)
    kl1, kl2, kl3 = jax.random.split(jax.random.fold_in(kl, 7), 3)
    full = T - 1 - jax.random.randint(kl1, (B,), 0, T // 8)
    tiny = jax.random.randint(kl2, (B,), 1, 9)
    lengths = jnp.where(jax.random.bernoulli(kl3, 0.5, (B,)), full, tiny).astype(jnp.int32)
    bf = jnp.bfloat16
    return {'x': x.astype(bf), 'Wq': Wq.astype(bf), 'Wk': Wk.astype(bf), 'Wv': Wv.astype(bf),
            'Wo': Wo.astype(bf), 'Kc': Kc.astype(bf), 'Vc': Vc.astype(bf), 'lengths': lengths}


def reference(x, Wq, Wk, Wv, Wo, Kc, Vc, lengths):
    scale = DH ** -0.5
    q = jnp.dot(x, Wq, preferred_element_type=jnp.float32).astype(jnp.bfloat16).reshape(B, H, DH)
    k_new = jnp.dot(x, Wk, preferred_element_type=jnp.float32).astype(jnp.bfloat16)
    v_new = jnp.dot(x, Wv, preferred_element_type=jnp.float32).astype(jnp.bfloat16)
    pos = jnp.arange(T)

    def one(a):
        qb, Kb, Vb, kn, vn, n = a
        s = jnp.dot(qb, Kb.T, preferred_element_type=jnp.float32) * scale
        s = jnp.where(pos[None, :] < n, s, -jnp.inf)
        sn = jnp.dot(qb, kn, preferred_element_type=jnp.float32) * scale
        m = jnp.maximum(jnp.max(s, axis=1), sn)
        p = jnp.exp(s - m[:, None])
        pn = jnp.exp(sn - m)
        l = jnp.sum(p, axis=1) + pn
        acc = jnp.dot(p.astype(jnp.bfloat16), Vb, preferred_element_type=jnp.float32)
        acc = acc + pn.astype(jnp.bfloat16).astype(jnp.float32)[:, None] * vn.astype(jnp.float32)[None, :]
        return (acc / l[:, None]).astype(jnp.bfloat16)

    o = lax.map(one, (q, Kc, Vc, k_new, v_new, lengths))
    y = x.astype(jnp.float32) + jnp.dot(o.reshape(B, H * DH), Wo, preferred_element_type=jnp.float32)
    return y.astype(jnp.bfloat16), k_new, v_new
```

```python
import functools

import jax
import jax.numpy as jnp
from jax import lax
from jax.experimental import pallas as pl
from jax.experimental.pallas import tpu as pltpu
from jax.sharding import PartitionSpec as P

MESH = pl.DeviceIdType.MESH
BK = 512
G = 4
RING = 6
AHEAD = 4
CH = 4
SUB = 2
NH = 8


def _vmem():
    return pl.BlockSpec(memory_space=pltpu.VMEM)


def _any():
    return pl.BlockSpec(memory_space=pl.ANY)


def _smem():
    return pl.BlockSpec(memory_space=pltpu.SMEM)


def _attn_kernel(scale, seqs, blks, lens, meta, q_ref, kn_ref, vn_ref, kc, vc, o_ref,
                 kbuf, vbuf, pbuf, mbuf, lbuf, mrun, lrun, arun, ksem, vsem):
    start = meta[0]
    steps = meta[1]

    def copies(g):
        slot = lax.rem(g, RING)
        out = []
        for u in range(G):
            n = g * G + u
            row = start + seqs[n] % q_ref.shape[0]
            span = pl.ds(pl.multiple_of(blks[n] * BK, BK), BK)
            out.append((pltpu.make_async_copy(kc.at[row, span], kbuf.at[slot, u], ksem.at[slot, u]),
                        pltpu.make_async_copy(vc.at[row, span], vbuf.at[slot, u], vsem.at[slot, u])))
        return out

    def fetch(g):
        for ck, cv in copies(g):
            ck.start()
            cv.start()

    def insert(buf, slot, u, row, new):
        base = pl.multiple_of(jnp.clip(row // 16, 0, BK // 16 - 1) * 16, 16)
        old = buf[slot, u, pl.ds(base, 16), :]
        at = lax.broadcasted_iota(jnp.int32, (16, 1), 0) + base == row
        buf[slot, u, pl.ds(base, 16), :] = jnp.where(at, new, old.astype(jnp.float32)).astype(jnp.bfloat16)

    def scores(g):
        slot = lax.rem(g, RING)
        half = lax.rem(g, 2)
        for ck, _ in copies(g):
            ck.wait()
        for u in range(G):
            n = g * G + u
            seq = seqs[n]
            sq = seq % q_ref.shape[0]
            row = lens[seq] - blks[n] * BK
            insert(kbuf, slot, u, row, kn_ref[sq].astype(jnp.float32))
            s = lax.dot_general(q_ref[sq], kbuf[slot, u], (((1,), (1,)), ((), ())),
                                preferred_element_type=jnp.float32) * scale
            s = jnp.where(lax.broadcasted_iota(jnp.int32, s.shape, 1) <= row, s, -jnp.inf)
            m = jnp.max(s, axis=1, keepdims=True)
            p = jnp.exp(s - m)
            pbuf[half, u] = p.astype(jnp.bfloat16)
            mbuf[half, u] = jnp.broadcast_to(m, mbuf.shape[2:])
            lbuf[half, u] = jnp.broadcast_to(jnp.sum(p, axis=1, keepdims=True), lbuf.shape[2:])

    def values(g):
        slot = lax.rem(g, RING)
        half = lax.rem(g, 2)
        for _, cv in copies(g):
            cv.wait()
        accs = []
        for u in range(G):
            n = g * G + u
            seq = seqs[n]
            row = lens[seq] - blks[n] * BK
            insert(vbuf, slot, u, row, vn_ref[seq % q_ref.shape[0]].astype(jnp.float32))
            accs.append(jnp.dot(pbuf[half, u], vbuf[slot, u], preferred_element_type=jnp.float32))
        mo, lo, ao = mrun[...], lrun[...], arun[...]
        for u in range(G):
            n = g * G + u
            first = blks[n] == 0
            mo = jnp.where(first, -1e30, mo)
            lo = jnp.where(first, 0.0, lo)
            ao = jnp.where(first, 0.0, ao)
            m = jnp.maximum(mo, mbuf[half, u])
            alpha = jnp.exp(mo - m)
            beta = jnp.exp(mbuf[half, u] - m)
            lo = lo * alpha + lbuf[half, u] * beta
            ao = ao * jnp.concatenate([alpha, alpha], 1) + accs[u] * jnp.concatenate([beta, beta], 1)
            mo = m
            inv = 1.0 / lo
            o_ref[seqs[n]] = (ao * jnp.concatenate([inv, inv], 1)).astype(jnp.bfloat16)
        mrun[...] = mo
        lrun[...] = lo
        arun[...] = ao

    mrun[...] = jnp.zeros_like(mrun)
    lrun[...] = jnp.zeros_like(lrun)
    arun[...] = jnp.zeros_like(arun)
    for g in range(AHEAD):
        @pl.when(g < steps)
        def _():
            fetch(g)

    @pl.when(AHEAD < steps)
    def _():
        fetch(AHEAD)

    scores(0)

    def body(g, c):
        @pl.when(g + AHEAD < steps)
        def _():
            fetch(g + AHEAD)

        values(g - 1)
        scores(g)
        return c

    lax.fori_loop(1, steps, body, 0)
    values(steps - 1)


def _attend(q, kn, vn, Kc, Vc, lens, start):
    nb, h, dh = q.shape
    t = Kc.shape[1]
    assert dh == 256 and t % BK == 0
    blocks = lens // BK + 1
    cum = jnp.sum(jnp.where(jnp.arange(nb)[None, :] <= jnp.arange(nb)[:, None], blocks[None, :], 0), axis=1)
    most = nb * (t // BK) + G
    n = jnp.arange(most)
    seqs = jnp.sum((cum[None, :] <= n[:, None]).astype(jnp.int32), axis=1)
    before = jnp.max(jnp.where(cum[None, :] <= n[:, None], cum[None, :], 0), axis=1)
    blks = jnp.where(seqs < nb, n - before, 0)
    steps = (cum[-1] + G - 1) // G
    meta = jnp.stack([start, steps]).astype(jnp.int32)
    lens1 = jnp.concatenate([lens, jnp.ones((8,), jnp.int32)])
    bf, f32 = jnp.bfloat16, jnp.float32
    out = pl.pallas_call(
        functools.partial(_attn_kernel, dh ** -0.5),
        out_shape=jax.ShapeDtypeStruct((nb + 1, h, dh), bf),
        in_specs=[_smem()] * 4 + [_vmem()] * 3 + [_any()] * 2,
        out_specs=_vmem(),
        scratch_shapes=[
            pltpu.VMEM((RING, G, BK, dh), bf), pltpu.VMEM((RING, G, BK, dh), bf),
            pltpu.VMEM((2, G, h, BK), bf), pltpu.VMEM((2, G, h, 128), f32), pltpu.VMEM((2, G, h, 128), f32),
            pltpu.VMEM((h, 128), f32), pltpu.VMEM((h, 128), f32), pltpu.VMEM((h, dh), f32),
            pltpu.SemaphoreType.DMA((RING, G)), pltpu.SemaphoreType.DMA((RING, G)),
        ],
        name="attend",
    )(seqs.astype(jnp.int32), blks.astype(jnp.int32), lens1, meta, q, kn.reshape(nb, 1, dh), vn.reshape(nb, 1, dh), Kc, Vc)
    return out[:nb]


def _out_kernel(ne, nm, o_ref, wo, x, y, wv, xv, ob, pown, psend, precv, ssend, srecv, ybuf, yrecv,
                wsem, xsem, lsem, osend, orecv, psend_s, precv_s, ssend_s, srecv_s,
                cs, cr, es, er, fs, fr):
    i = lax.axis_index("emb")
    j = lax.axis_index("model")
    me = i * nm + j
    c = lax.rem(j, 2)
    jp = j + 1 - 2 * c
    jx = lax.rem(j + 2, nm)
    ie = 1 - i
    half = wv.shape[2]
    cw = half // SUB
    rows = o_ref.shape[0] // CH
    kk = wv.shape[1]
    dev = ne * nm

    def at(a, b):
        return {"emb": a, "model": b}

    barrier = pltpu.get_barrier_semaphore()
    for r in range(1, dev):
        d = lax.rem(me + r, dev)
        pl.semaphore_signal(barrier, inc=1, device_id=at(d // nm, lax.rem(d, nm)), device_id_type=MESH)
    pl.semaphore_wait(barrier, dev - 1)

    def osend_copy(s, r):
        d = lax.rem(me + r, dev)
        dj = lax.rem(d, nm)
        return pltpu.make_async_remote_copy(
            src_ref=o_ref.at[pl.ds(pl.multiple_of(s * rows, rows), rows), pl.ds(pl.multiple_of(dj * kk, kk), kk)],
            dst_ref=ob.at[s, pl.ds(pl.multiple_of(me * rows, rows), rows), :],
            send_sem=osend.at[s, r], recv_sem=orecv.at[s, dev - r],
            device_id=at(d // nm, dj), device_id_type=MESH)

    def orecv_copy(s, r):
        d = lax.rem(me + r, dev)
        return pltpu.make_async_remote_copy(
            src_ref=ob.at[s, pl.ds(pl.multiple_of(d * rows, rows), rows), :],
            dst_ref=ob.at[s, pl.ds(pl.multiple_of(d * rows, rows), rows), :],
            send_sem=osend.at[s, r], recv_sem=orecv.at[s, r],
            device_id=at(d // nm, lax.rem(d, nm)), device_id_type=MESH)

    for s in range(CH):
        for r in (4, 6, 5, 7, 2, 3, 1):
            osend_copy(s, r).start()

    def wcopy(b, u):
        col = pl.multiple_of((1 - c if b == 0 else c) * half + u * cw, cw)
        return pltpu.make_async_copy(wo.at[:, pl.ds(col, cw)], wv.at[b, :, pl.ds(u * cw, cw)], wsem.at[b, u])

    for b in range(2):
        for u in range(SUB):
            wcopy(b, u).start()
    mycol = pl.multiple_of((i * 2 + c) * half, half)
    excol = pl.multiple_of(((1 - i) * 2 + c) * half, half)
    xcopy = pltpu.make_async_copy(x.at[:, :, pl.ds(mycol, half)], xv, xsem)
    xcopy.start()
    for s in range(CH):
        ob[s, pl.ds(pl.multiple_of(me * rows, rows), rows), :] = o_ref[
            pl.ds(s * rows, rows), pl.ds(pl.multiple_of(j * kk, kk), kk)]
    for b in range(2):
        for u in range(SUB):
            wcopy(b, u).wait()
    xcopy.wait()

    def pcopy(s, u):
        return pltpu.make_async_remote_copy(
            src_ref=psend.at[s, u], dst_ref=precv.at[s, u], send_sem=psend_s.at[s, u], recv_sem=precv_s.at[s, u],
            device_id=at(i, jp), device_id_type=MESH)

    def scopy(s, u):
        return pltpu.make_async_remote_copy(
            src_ref=ssend.at[s, u], dst_ref=srecv.at[s, u], send_sem=ssend_s.at[s, u], recv_sem=srecv_s.at[s, u],
            device_id=at(i, jx), device_id_type=MESH)

    def yref(s, u, base):
        return y.at[:, pl.ds(pl.multiple_of(s * rows, rows), rows), pl.ds(pl.multiple_of(base + u * cw, cw), cw)]

    def ccopy(s, u):
        return pltpu.make_async_remote_copy(
            src_ref=ybuf.at[s, u], dst_ref=yref(s, u, mycol), send_sem=cs.at[s, u], recv_sem=cr.at[s, u],
            device_id=at(i, jp), device_id_type=MESH)

    def ecopy(s, u):
        return pltpu.make_async_remote_copy(
            src_ref=ybuf.at[s, u], dst_ref=yrecv.at[s, u], send_sem=es.at[s, u], recv_sem=er.at[s, u],
            device_id=at(ie, j), device_id_type=MESH)

    def fcopy(s, u):
        return pltpu.make_async_remote_copy(
            src_ref=yrecv.at[s, u], dst_ref=yref(s, u, excol), send_sem=fs.at[s, u], recv_sem=fr.at[s, u],
            device_id=at(i, jp), device_id_type=MESH)

    def lcopy(s, u, k):
        if k == 0:
            return pltpu.make_async_copy(ybuf.at[s, u], yref(s, u, mycol), lsem.at[0, s, u])
        return pltpu.make_async_copy(yrecv.at[s, u], yref(s, u, excol), lsem.at[1, s, u])

    def compute(s):
        for r in range(1, dev):
            orecv_copy(s, r).wait_recv()
        lhs = ob[s]
        for u in range(SUB):
            psend[s, u] = jnp.dot(lhs, wv[0, :, u * cw:(u + 1) * cw],
                                  preferred_element_type=jnp.float32).astype(jnp.bfloat16)
            pcopy(s, u).start()
        for u in range(SUB):
            pown[u] = jnp.dot(lhs, wv[1, :, u * cw:(u + 1) * cw], preferred_element_type=jnp.float32)
        for u in range(SUB):
            pcopy(s, u).wait_recv()
            ssend[s, u] = (pown[u] + precv[s, u].astype(jnp.float32)).astype(jnp.bfloat16)
            scopy(s, u).start()

    def finish(s):
        for u in range(SUB):
            scopy(s, u).wait_recv()
            tot = ssend[s, u].astype(jnp.float32) + srecv[s, u].astype(jnp.float32)
            xs = xv[:, pl.ds(pl.multiple_of(s * rows, rows), rows), u * cw:(u + 1) * cw].astype(jnp.float32)
            ybuf[s, u] = (xs + tot.reshape(dev, rows, cw)).astype(jnp.bfloat16)
            ecopy(s, u).start()
            ccopy(s, u).start()
            lcopy(s, u, 0).start()

    def forward(s):
        for u in range(SUB):
            ecopy(s, u).wait_recv()
            fcopy(s, u).start()
            lcopy(s, u, 1).start()

    def step(s, carry):
        compute(s)

        @pl.when(s >= 1)
        def _():
            finish(s - 1)

        @pl.when(s >= 2)
        def _():
            forward(s - 2)

        return carry

    lax.fori_loop(0, CH, step, 0)
    finish(CH - 1)
    forward(CH - 2)
    forward(CH - 1)
    for s in range(CH):
        for r in range(1, dev):
            osend_copy(s, r).wait_send()
        for u in range(SUB):
            pcopy(s, u).wait_send()
            scopy(s, u).wait_send()
            ecopy(s, u).wait_send()
            ccopy(s, u).wait()
            fcopy(s, u).wait()
            lcopy(s, u, 0).wait()
            lcopy(s, u, 1).wait()


def _project_out(o, Wo, x, ne, nm):
    bl, full = o.shape
    kk, ncol = Wo.shape
    half = ncol // 2
    dev = ne * nm
    rows = bl // CH
    cw = half // SUB
    b, d = x.shape
    bf, f32 = jnp.bfloat16, jnp.float32
    dma = pltpu.SemaphoreType.DMA
    pieces = pltpu.VMEM((CH, SUB, dev * rows, cw), bf)
    pieces3 = pltpu.VMEM((CH, SUB, dev, rows, cw), bf)
    pair = [dma((CH, SUB)), dma((CH, SUB))]
    y = pl.pallas_call(
        functools.partial(_out_kernel, ne, nm),
        out_shape=jax.ShapeDtypeStruct((dev, bl, d), bf),
        in_specs=[_vmem(), _any(), _any()],
        out_specs=_any(),
        scratch_shapes=[
            pltpu.VMEM((2, kk, half), bf), pltpu.VMEM((dev, bl, half), bf), pltpu.VMEM((CH, dev * rows, kk), bf),
            pltpu.VMEM((SUB, dev * rows, cw), f32), pieces, pieces, pieces, pieces, pieces3, pieces3,
            dma((2, SUB)), dma, dma((2, CH, SUB)), dma((CH, dev)), dma((CH, dev)),
        ] + pair * 5,
        compiler_params=pltpu.CompilerParams(collective_id=1, has_side_effects=True, vmem_limit_bytes=60 << 20),
        name="project_out",
    )(o, Wo, x.reshape(dev, bl, d))
    return y.reshape(b, d)


def _in_kernel(ne, nm, x, wq, wk, wv, q, k_out, v_out, xv, wqv, wkv, qsend, qrecv, qown, qb,
               xsem, wsem, ksem, ss, sr, hs, hr, ls):
    i = lax.axis_index("emb")
    j = lax.axis_index("model")
    ie = 1 - i
    de = wq.shape[0]
    be = xv.shape[1] // 2
    bl = be // nm
    cw = wq.shape[1] // NH
    dh = wk.shape[1]

    def at(a, b):
        return {"emb": a, "model": b}

    def xcopy(a, r):
        row = pl.multiple_of((ie if a == 0 else i) * be, be)
        col = pl.multiple_of((i if r == 0 else ie) * de, de)
        return pltpu.make_async_copy(x.at[pl.ds(row, be), pl.ds(col, de)], xv.at[r, a * be:(a + 1) * be, :], xsem.at[a, r])

    def wcopy(h):
        return pltpu.make_async_copy(wq.at[:, pl.ds(h * cw, cw)], wqv.at[h], wsem.at[h])

    def kcopy(n, r):
        src = wk if n == 0 else wv
        row = pl.multiple_of((i if r == 0 else ie) * de, de)
        return pltpu.make_async_copy(src.at[pl.ds(row, de), :], wkv.at[n, r], ksem.at[n, r])

    xcopy(0, 0).start()
    for h in range(NH):
        wcopy(h).start()
    xcopy(1, 0).start()
    xcopy(0, 1).start()
    xcopy(1, 1).start()
    for n in range(2):
        for r in range(2):
            kcopy(n, r).start()

    barrier = pltpu.get_barrier_semaphore()
    pl.semaphore_signal(barrier, inc=1, device_id=at(ie, j), device_id_type=MESH)
    for r in range(1, nm):
        pl.semaphore_signal(barrier, inc=1, device_id=at(i, lax.rem(j + r, nm)), device_id_type=MESH)
    pl.semaphore_wait(barrier, nm)

    def scopy(h):
        return pltpu.make_async_remote_copy(
            src_ref=qsend.at[h], dst_ref=qrecv.at[h], send_sem=ss.at[h], recv_sem=sr.at[h],
            device_id=at(ie, j), device_id_type=MESH)

    def hcopy(h, r):
        d = lax.rem(j + r, nm)
        return pltpu.make_async_remote_copy(
            src_ref=qb.at[h, pl.ds(pl.multiple_of(d * bl, bl), bl), :],
            dst_ref=q.at[:, pl.ds(pl.multiple_of((j * NH + h) * cw, cw), cw)],
            send_sem=hs.at[h, r], recv_sem=hr.at[h, nm - r],
            device_id=at(i, d), device_id_type=MESH)

    def hrecv(h, r):
        d = lax.rem(j + r, nm)
        return pltpu.make_async_remote_copy(
            src_ref=qb.at[h, pl.ds(0, bl), :],
            dst_ref=q.at[:, pl.ds(pl.multiple_of((d * NH + h) * cw, cw), cw)],
            send_sem=hs.at[h, r], recv_sem=hr.at[h, r],
            device_id=at(i, d), device_id_type=MESH)

    def hself(h):
        return pltpu.make_async_copy(
            qb.at[h, pl.ds(pl.multiple_of(j * bl, bl), bl), :],
            q.at[:, pl.ds(pl.multiple_of((j * NH + h) * cw, cw), cw)], ls.at[h])

    xcopy(0, 0).wait()
    for h in range(NH):
        wcopy(h).wait()
        qsend[h] = jnp.dot(xv[0, :be, :], wqv[h], preferred_element_type=jnp.float32)
        scopy(h).start()
    xcopy(1, 0).wait()
    for h in range(NH):
        qown[h] = jnp.dot(xv[0, be:, :], wqv[h], preferred_element_type=jnp.float32)

    xcopy(0, 1).wait()
    xcopy(1, 1).wait()
    for n in range(2):
        for r in range(2):
            kcopy(n, r).wait()
    for n, out in ((0, k_out), (1, v_out)):
        for a in range(2):
            acc = jnp.dot(xv[0, a * be:(a + 1) * be, :], wkv[n, 0], preferred_element_type=jnp.float32)
            acc += jnp.dot(xv[1, a * be:(a + 1) * be, :], wkv[n, 1], preferred_element_type=jnp.float32)
            out[pl.ds(pl.multiple_of((ie if a == 0 else i) * be, be), be), :] = acc.astype(jnp.bfloat16)

    for h in range(NH):
        scopy(h).wait_recv()
        qb[h] = (qown[h] + qrecv[h]).astype(jnp.bfloat16)
        for r in (2, 3, 1):
            hcopy(h, r).start()
        hself(h).start()
    for h in range(NH):
        scopy(h).wait_send()
        hself(h).wait()
        for r in range(1, nm):
            hcopy(h, r).wait_send()
            hrecv(h, r).wait_recv()


def _project_in(x, Wq, Wk, Wv, ne, nm):
    b, d = x.shape
    de, hw = Wq.shape
    dh = Wk.shape[1]
    be = b // ne
    bl = be // nm
    cw = hw // NH
    bf, f32 = jnp.bfloat16, jnp.float32
    dma = pltpu.SemaphoreType.DMA
    return pl.pallas_call(
        functools.partial(_in_kernel, ne, nm),
        out_shape=(jax.ShapeDtypeStruct((bl, hw * nm), bf), jax.ShapeDtypeStruct((b, dh), bf),
                   jax.ShapeDtypeStruct((b, dh), bf)),
        in_specs=[_any()] * 4,
        out_specs=(_any(), _vmem(), _vmem()),
        scratch_shapes=[
            pltpu.VMEM((2, b, de), bf), pltpu.VMEM((NH, de, cw), bf), pltpu.VMEM((2, 2, de, dh), bf),
            pltpu.VMEM((NH, be, cw), f32), pltpu.VMEM((NH, be, cw), f32), pltpu.VMEM((NH, be, cw), f32),
            pltpu.VMEM((NH, be, cw), bf),
            dma((2, 2)), dma((NH,)), dma((2, 2)), dma((NH,)), dma((NH,)), dma((NH, nm)), dma((NH, nm)), dma((NH,)),
        ],
        compiler_params=pltpu.CompilerParams(collective_id=0, has_side_effects=True, vmem_limit_bytes=60 << 20),
        name="project_in",
    )(x, Wq, Wk, Wv)


def solution(mesh):
    ne = mesh.shape['emb']
    nm = mesh.shape['model']

    def local(x, Wq, Wk, Wv, Wo, Kc, Vc, lengths):
        b, d = x.shape
        dh = Wk.shape[1]
        heads = Wq.shape[1] // dh * nm
        be = b // ne
        bl = be // nm
        i = lax.axis_index('emb')
        j = lax.axis_index('model')
        start = i * be + j * bl
        q, k_new, v_new = _project_in(x, Wq, Wk, Wv, ne, nm)
        kn = lax.dynamic_slice_in_dim(k_new, start, bl, 0)
        vn = lax.dynamic_slice_in_dim(v_new, start, bl, 0)
        lens = lax.dynamic_slice_in_dim(lengths, start, bl, 0)
        o = _attend(q.reshape(bl, heads, dh), kn, vn, Kc, Vc, lens, start)
        y = _project_out(o.reshape(bl, heads * dh), Wo, x, ne, nm)
        return y, k_new, v_new

    in_specs = (P('rep', None), P('emb', 'model'), P(), P(), P('model', 'emb'),
                P('rep', None, None), P('rep', None, None), P('rep'))
    out_specs = (P('rep', None), P('rep', None), P('rep', None))
    return jax.shard_map(local, mesh=mesh, in_specs=in_specs, out_specs=out_specs, check_vma=False)
```

```python
import functools

import jax
import jax.numpy as jnp
from jax import lax
from jax.experimental import pallas as pl
from jax.experimental.pallas import tpu as pltpu
from jax.sharding import PartitionSpec as P

MESH = pl.DeviceIdType.MESH
BK = 512
G = 4
RING = 6
AHEAD = 4
CH = 4
SUB = 4
NH = 8


def _vmem():
    return pl.BlockSpec(memory_space=pltpu.VMEM)


def _any():
    return pl.BlockSpec(memory_space=pl.ANY)


def _smem():
    return pl.BlockSpec(memory_space=pltpu.SMEM)


def _attn_kernel(scale, nm, lens, q_ref, kn_ref, vn_ref, kc, vc, o_ref, ko_ref, vo_ref,
                 seqs, blks, qa, qb, oa, ob, knf, vnf, kbuf, vbuf, pbuf, mbuf, lbuf, mrun, lrun, arun, ksem, vsem):
    nb = q_ref.shape[0]
    dh = kn_ref.shape[1]
    nh = q_ref.shape[1] // dh
    per = kc.shape[1] // BK
    start = (lax.axis_index("emb") * nm + lax.axis_index("model")) * nb

    def listed(sq, n):
        for t in range(per):
            seqs[n + t] = sq
            blks[n + t] = t
        return n + lens[start + sq] // BK + 1

    total = lax.fori_loop(0, nb, listed, 0, unroll=4)
    for t in range(G):
        seqs[total + t] = nb
        blks[total + t] = 0
    steps = (total + G - 1) // G

    def copies(g):
        slot = lax.rem(g, RING)
        out = []
        for u in range(G):
            n = g * G + u
            row = start + jnp.minimum(seqs[n], nb - 1)
            span = pl.ds(pl.multiple_of(blks[n] * BK, BK), BK)
            out.append((pltpu.make_async_copy(kc.at[row, span], kbuf.at[slot, u], ksem.at[slot, u]),
                        pltpu.make_async_copy(vc.at[row, span], vbuf.at[slot, u], vsem.at[slot, u])))
        return out

    def fetch(g):
        for ck, cv in copies(g):
            ck.start()
            cv.start()

    def landed(g, which):
        slot = lax.rem(g, RING)
        buf, sem, src = ((kbuf, ksem, kc), (vbuf, vsem, vc))[which]
        for u in range(G):
            pltpu.make_async_copy(src.at[0, pl.ds(0, BK)], buf.at[slot, u], sem.at[slot, u]).wait()

    def insert(buf, slot, u, row, new):
        base = pl.multiple_of(jnp.clip(row // 16, 0, BK // 16 - 1) * 16, 16)
        old = buf[slot, u, pl.ds(base, 16), :]
        at = lax.broadcasted_iota(jnp.int32, (16, 1), 0) + base == row
        buf[slot, u, pl.ds(base, 16), :] = jnp.where(at, new, old.astype(jnp.float32)).astype(jnp.bfloat16)

    def item(g, u):
        n = g * G + u
        seq = seqs[n]
        sq = jnp.minimum(seq, nb - 1)
        return seq, sq, blks[n], lens[start + sq] - blks[n] * BK

    def scores(g):
        slot = lax.rem(g, RING)
        half = lax.rem(g, 2)
        for u in range(G):
            _, sq, _, row = item(g, u)
            insert(kbuf, slot, u, row, knf[pl.ds(sq, 1), :])
            at = pl.ds(pl.multiple_of(sq * nh, nh), nh)
            qs = jnp.concatenate([qa[at, :], qb[at, :]], 1).astype(jnp.bfloat16)
            s = lax.dot_general(qs, kbuf[slot, u], (((1,), (1,)), ((), ())),
                                preferred_element_type=jnp.float32) * scale
            s = jnp.where(lax.broadcasted_iota(jnp.int32, s.shape, 1) <= row, s, -jnp.inf)
            m = jnp.max(s, axis=1, keepdims=True)
            p = jnp.exp(s - m)
            pbuf[half, u] = p.astype(jnp.bfloat16)
            mbuf[half, u] = jnp.broadcast_to(m, mbuf.shape[2:])
            lbuf[half, u] = jnp.broadcast_to(jnp.sum(p, axis=1, keepdims=True), lbuf.shape[2:])

    def values(g):
        slot = lax.rem(g, RING)
        half = lax.rem(g, 2)
        accs = []
        for u in range(G):
            _, sq, _, row = item(g, u)
            insert(vbuf, slot, u, row, vnf[pl.ds(sq, 1), :])
            accs.append(jnp.dot(pbuf[half, u], vbuf[slot, u], preferred_element_type=jnp.float32))
        mo, lo, ao = mrun[...], lrun[...], arun[...]
        for u in range(G):
            seq, _, blk, _ = item(g, u)
            first = blk == 0
            mo = jnp.where(first, -1e30, mo)
            lo = jnp.where(first, 0.0, lo)
            ao = jnp.where(first, 0.0, ao)
            m = jnp.maximum(mo, mbuf[half, u])
            alpha = jnp.exp(mo - m)
            beta = jnp.exp(mbuf[half, u] - m)
            lo = lo * alpha + lbuf[half, u] * beta
            ao = ao * jnp.concatenate([alpha, alpha], 1) + accs[u] * jnp.concatenate([beta, beta], 1)
            mo = m
            inv = 1.0 / lo
            at = pl.ds(pl.multiple_of(seq * nh, nh), nh)
            oa[at, :] = ao[:, :128] * inv
            ob[at, :] = ao[:, 128:] * inv
        mrun[...] = mo
        lrun[...] = lo
        arun[...] = ao

    for g in range(AHEAD + 1):
        @pl.when(g < steps)
        def _():
            fetch(g)

    mrun[...] = jnp.zeros_like(mrun)
    lrun[...] = jnp.zeros_like(lrun)
    arun[...] = jnp.zeros_like(arun)
    mine = pl.ds(pl.multiple_of(start, nb), nb)
    knf[...] = kn_ref[mine, :].astype(jnp.float32)
    vnf[...] = vn_ref[mine, :].astype(jnp.float32)
    for h in range(nh):
        qa[pl.ds(h, nb, stride=nh), :] = q_ref[:, h * dh:h * dh + 128].astype(jnp.float32)
        qb[pl.ds(h, nb, stride=nh), :] = q_ref[:, h * dh + 128:(h + 1) * dh].astype(jnp.float32)
    ko_ref[...] = kn_ref[...]
    vo_ref[...] = vn_ref[...]

    landed(0, 0)
    scores(0)

    def body(g, c):
        @pl.when(g + AHEAD < steps)
        def _():
            fetch(g + AHEAD)

        landed(g - 1, 1)
        landed(g, 0)
        values(g - 1)
        scores(g)
        return c

    lax.fori_loop(1, steps, body, 0)
    landed(steps - 1, 1)
    values(steps - 1)
    for h in range(nh):
        o_ref[:, h * dh:h * dh + 128] = oa[pl.ds(h, nb, stride=nh), :].astype(jnp.bfloat16)
        o_ref[:, h * dh + 128:(h + 1) * dh] = ob[pl.ds(h, nb, stride=nh), :].astype(jnp.bfloat16)


def _attend(q, k_new, v_new, Kc, Vc, lengths, nm):
    nb, full = q.shape
    t, dh = Kc.shape[1:]
    h = full // dh
    assert dh == 256 and t % BK == 0
    most = nb * (t // BK) + 2 * G
    bf, f32 = jnp.bfloat16, jnp.float32
    kv = jax.ShapeDtypeStruct(k_new.shape, bf)
    return pl.pallas_call(
        functools.partial(_attn_kernel, dh ** -0.5, nm),
        out_shape=(jax.ShapeDtypeStruct((nb, full), bf), kv, kv),
        in_specs=[_smem()] + [_vmem()] * 3 + [_any()] * 2,
        out_specs=(_vmem(), _vmem(), _vmem()),
        scratch_shapes=[
            pltpu.SMEM((most,), jnp.int32), pltpu.SMEM((most,), jnp.int32),
            pltpu.VMEM((nb * h, 128), f32), pltpu.VMEM((nb * h, 128), f32),
            pltpu.VMEM((nb * h + h, 128), f32), pltpu.VMEM((nb * h + h, 128), f32),
            pltpu.VMEM((nb, dh), f32), pltpu.VMEM((nb, dh), f32),
            pltpu.VMEM((RING, G, BK, dh), bf), pltpu.VMEM((RING, G, BK, dh), bf),
            pltpu.VMEM((2, G, h, BK), bf), pltpu.VMEM((2, G, h, 128), f32), pltpu.VMEM((2, G, h, 128), f32),
            pltpu.VMEM((h, 128), f32), pltpu.VMEM((h, 128), f32), pltpu.VMEM((h, dh), f32),
            pltpu.SemaphoreType.DMA((RING, G)), pltpu.SemaphoreType.DMA((RING, G)),
        ],
        compiler_params=pltpu.CompilerParams(vmem_limit_bytes=40 << 20),
        name="attend",
    )(lengths, q, k_new, v_new, Kc, Vc)


def _out_kernel(ne, nm, o_ref, wo, x, y, wv, xv, ob, pown, psend, precv, ssend, srecv,
                wsem, xsem, osend, orecv, vsend, vrecv, ps, pr, xs_, xr, cs, cr, es, er, fs, fr):
    i = lax.axis_index("emb")
    j = lax.axis_index("model")
    c = lax.rem(j, 2)
    jp = j + 1 - 2 * c
    jx = lax.rem(j + 2, nm)
    ie = 1 - i
    half = wv.shape[2]
    cw = half // SUB
    rows = o_ref.shape[0] // CH
    kk = wv.shape[1]
    dev = ne * nm

    def at(a, b):
        return {"emb": a, "model": b}

    def wcopy(b, u):
        col = pl.multiple_of((1 - c if b == 0 else c) * half + u * cw, cw)
        return pltpu.make_async_copy(wo.at[:, pl.ds(col, cw)], wv.at[b, :, pl.ds(u * cw, cw)], wsem.at[b, u])

    for b in range(2):
        for u in range(SUB):
            wcopy(b, u).start()
    mycol = pl.multiple_of((i * 2 + c) * half, half)
    excol = pl.multiple_of((ie * 2 + c) * half, half)
    xcopy = pltpu.make_async_copy(x.at[:, :, pl.ds(mycol, half)], xv, xsem)
    xcopy.start()

    barrier = pltpu.get_barrier_semaphore()
    pl.semaphore_signal(barrier, inc=1, device_id=at(ie, j), device_id_type=MESH)
    for r in range(1, nm):
        pl.semaphore_signal(barrier, inc=1, device_id=at(i, lax.rem(j + r, nm)), device_id_type=MESH)
    pl.semaphore_wait(barrier, nm)

    def ocopy(s, r):
        d = lax.rem(j + r, nm)
        return pltpu.make_async_remote_copy(
            src_ref=o_ref.at[pl.ds(s * rows, rows), pl.ds(pl.multiple_of(d * kk, kk), kk)],
            dst_ref=ob.at[s, pl.ds(pl.multiple_of((i * nm + j) * rows, rows), rows), :],
            send_sem=osend.at[s, r], recv_sem=orecv.at[s, nm - r],
            device_id=at(i, d), device_id_type=MESH)

    def orecv_copy(s, r):
        d = lax.rem(j + r, nm)
        blk = ob.at[s, pl.ds(pl.multiple_of((i * nm + d) * rows, rows), rows), :]
        return pltpu.make_async_remote_copy(
            src_ref=blk, dst_ref=blk, send_sem=osend.at[s, r], recv_sem=orecv.at[s, r],
            device_id=at(i, d), device_id_type=MESH)

    def vcopy(s, r):
        dst = ob.at[s, pl.ds(pl.multiple_of((i * nm + lax.rem(j + r, nm)) * rows, rows), rows), :]
        src = o_ref.at[pl.ds(s * rows, rows), pl.ds(pl.multiple_of(j * kk, kk), kk)] if r == 0 else dst
        return pltpu.make_async_remote_copy(
            src_ref=src, dst_ref=dst, send_sem=vsend.at[s, r], recv_sem=vrecv.at[s, r],
            device_id=at(ie, j), device_id_type=MESH)

    def vrecv_copy(s, r):
        blk = ob.at[s, pl.ds(pl.multiple_of((ie * nm + lax.rem(j + r, nm)) * rows, rows), rows), :]
        return pltpu.make_async_remote_copy(
            src_ref=blk, dst_ref=blk, send_sem=vsend.at[s, r], recv_sem=vrecv.at[s, r],
            device_id=at(ie, j), device_id_type=MESH)

    for s in range(CH):
        for r in (2, 3, 1):
            ocopy(s, r).start()
    vcopy(0, 0).start()
    for s in range(CH):
        ob[s, pl.ds(pl.multiple_of((i * nm + j) * rows, rows), rows), :] = o_ref[
            pl.ds(s * rows, rows), pl.ds(pl.multiple_of(j * kk, kk), kk)]

    def relay(s):
        for r in (1, 2, 3):
            orecv_copy(s, r).wait_recv()
            vcopy(s, r).start()

    relay(0)
    vcopy(1, 0).start()
    relay(1)

    def pcopy(s, u):
        return pltpu.make_async_remote_copy(
            src_ref=psend.at[s, u], dst_ref=precv.at[s, u], send_sem=ps.at[s, u], recv_sem=pr.at[s, u],
            device_id=at(i, jp), device_id_type=MESH)

    def scopy(s, u):
        return pltpu.make_async_remote_copy(
            src_ref=ssend.at[s, u], dst_ref=srecv.at[s, u], send_sem=xs_.at[s, u], recv_sem=xr.at[s, u],
            device_id=at(i, jx), device_id_type=MESH)

    def piece(s, u, base):
        return y.at[:, pl.ds(pl.multiple_of(s * rows, rows), rows), pl.ds(pl.multiple_of(base + u * cw, cw), cw)]

    def ccopy(s, u):
        return pltpu.make_async_remote_copy(
            src_ref=piece(s, u, mycol), dst_ref=piece(s, u, mycol), send_sem=cs.at[s, u], recv_sem=cr.at[s, u],
            device_id=at(i, jp), device_id_type=MESH)

    def ecopy(s, u):
        return pltpu.make_async_remote_copy(
            src_ref=piece(s, u, mycol), dst_ref=piece(s, u, mycol), send_sem=es.at[s, u], recv_sem=er.at[s, u],
            device_id=at(ie, j), device_id_type=MESH)

    def fcopy(s, u):
        return pltpu.make_async_remote_copy(
            src_ref=piece(s, u, excol), dst_ref=piece(s, u, excol), send_sem=fs.at[s, u], recv_sem=fr.at[s, u],
            device_id=at(i, jp), device_id_type=MESH)

    for b in range(2):
        for u in range(SUB):
            wcopy(b, u).wait()
    xcopy.wait()

    def compute(s):
        for r in range(nm):
            vrecv_copy(s, r).wait_recv()
        lhs = ob[s]
        for u in range(SUB):
            psend[s, u] = jnp.dot(lhs, wv[0, :, u * cw:(u + 1) * cw],
                                  preferred_element_type=jnp.float32).astype(jnp.bfloat16)
            pcopy(s, u).start()
        for u in range(SUB):
            pown[u] = jnp.dot(lhs, wv[1, :, u * cw:(u + 1) * cw], preferred_element_type=jnp.float32)
            pcopy(s, u).wait_recv()
            ssend[s, u] = (pown[u] + precv[s, u].astype(jnp.float32)).astype(jnp.bfloat16)
            scopy(s, u).start()

    def finish(s):
        at_rows = pl.ds(pl.multiple_of(s * rows, rows), rows)
        for u in range(SUB):
            scopy(s, u).wait_recv()
            tot = ssend[s, u].astype(jnp.float32) + srecv[s, u].astype(jnp.float32)
            xs = xv[:, at_rows, u * cw:(u + 1) * cw].astype(jnp.float32)
            y[:, at_rows, pl.ds(pl.multiple_of(mycol + u * cw, cw), cw)] = (
                xs + tot.reshape(dev, rows, cw)).astype(jnp.bfloat16)
            ecopy(s, u).start()
            ccopy(s, u).start()

    def forward(s):
        for u in range(SUB):
            ecopy(s, u).wait_recv()
            fcopy(s, u).start()

    def step(s, carry):
        compute(s)

        @pl.when(s + 2 < CH)
        def _():
            vcopy_late(s + 2)

        @pl.when(s >= 1)
        def _():
            finish(s - 1)

        @pl.when(s >= 2)
        def _():
            forward(s - 2)

        return carry

    def vcopy_late(s):
        at_rows = pl.ds(pl.multiple_of(s * rows, rows), rows)
        own = pl.ds(pl.multiple_of((i * nm + j) * rows, rows), rows)
        pltpu.make_async_remote_copy(
            src_ref=o_ref.at[at_rows, pl.ds(pl.multiple_of(j * kk, kk), kk)], dst_ref=ob.at[s, own, :],
            send_sem=vsend.at[s, 0], recv_sem=vrecv.at[s, 0], device_id=at(ie, j), device_id_type=MESH).start()
        relay(s)

    lax.fori_loop(0, CH, step, 0)
    finish(CH - 1)
    forward(CH - 2)
    forward(CH - 1)
    for s in range(CH):
        for r in range(1, nm):
            ocopy(s, r).wait_send()
        for r in range(nm):
            vcopy(s, r).wait_send()
        for u in range(SUB):
            pcopy(s, u).wait_send()
            scopy(s, u).wait_send()
            ecopy(s, u).wait_send()
            ccopy(s, u).wait()
            fcopy(s, u).wait()


def _project_out(o, Wo, x, ne, nm):
    bl, full = o.shape
    kk, ncol = Wo.shape
    half = ncol // 2
    dev = ne * nm
    rows = bl // CH
    cw = half // SUB
    b, d = x.shape
    bf, f32 = jnp.bfloat16, jnp.float32
    dma = pltpu.SemaphoreType.DMA
    pieces = pltpu.VMEM((CH, SUB, dev * rows, cw), bf)
    y = pl.pallas_call(
        functools.partial(_out_kernel, ne, nm),
        out_shape=pltpu.VMEM((dev, bl, d), bf),
        in_specs=[_vmem(), _any(), _any()],
        out_specs=_vmem(),
        scratch_shapes=[
            pltpu.VMEM((2, kk, half), bf), pltpu.VMEM((dev, bl, half), bf), pltpu.VMEM((CH, dev * rows, kk), bf),
            pltpu.VMEM((SUB, dev * rows, cw), f32), pieces, pieces, pieces, pieces,
            dma((2, SUB)), dma,
        ] + [dma((CH, nm))] * 4 + [dma((CH, SUB))] * 10,
        compiler_params=pltpu.CompilerParams(collective_id=1, has_side_effects=True, vmem_limit_bytes=36 << 20),
        name="project_out",
    )(o, Wo, x.reshape(dev, bl, d))
    return y.reshape(b, d)


def _in_kernel(ne, nm, x, wq, wk, wv, q, k_out, v_out, xv, wqv, wkv, qsend, qrecv, qown, qb,
               xsem, wsem, ksem, ss, sr, hs, hr, ls):
    i = lax.axis_index("emb")
    j = lax.axis_index("model")
    ie = 1 - i
    de = wq.shape[0]
    be = xv.shape[1] // 2
    bl = be // nm
    cw = wq.shape[1] // NH
    dh = wk.shape[1]

    def at(a, b):
        return {"emb": a, "model": b}

    def xcopy(a, r):
        row = pl.multiple_of((ie if a == 0 else i) * be, be)
        col = pl.multiple_of((i if r == 0 else ie) * de, de)
        return pltpu.make_async_copy(x.at[pl.ds(row, be), pl.ds(col, de)], xv.at[r, a * be:(a + 1) * be, :], xsem.at[a, r])

    def wcopy(h):
        return pltpu.make_async_copy(wq.at[:, pl.ds(h * cw, cw)], wqv.at[h], wsem.at[h])

    def kcopy(n, r):
        src = wk if n == 0 else wv
        row = pl.multiple_of((i if r == 0 else ie) * de, de)
        return pltpu.make_async_copy(src.at[pl.ds(row, de), :], wkv.at[n, r], ksem.at[n, r])

    xcopy(0, 0).start()
    for h in range(NH):
        wcopy(h).start()
    xcopy(1, 0).start()
    xcopy(0, 1).start()
    xcopy(1, 1).start()
    for n in range(2):
        for r in range(2):
            kcopy(n, r).start()

    barrier = pltpu.get_barrier_semaphore()
    pl.semaphore_signal(barrier, inc=1, device_id=at(ie, j), device_id_type=MESH)
    for r in range(1, nm):
        pl.semaphore_signal(barrier, inc=1, device_id=at(i, lax.rem(j + r, nm)), device_id_type=MESH)
    pl.semaphore_wait(barrier, nm)

    def scopy(h):
        return pltpu.make_async_remote_copy(
            src_ref=qsend.at[h], dst_ref=qrecv.at[h], send_sem=ss.at[h], recv_sem=sr.at[h],
            device_id=at(ie, j), device_id_type=MESH)

    def hcopy(h, r):
        d = lax.rem(j + r, nm)
        return pltpu.make_async_remote_copy(
            src_ref=qb.at[h, pl.ds(pl.multiple_of(d * bl, bl), bl), :],
            dst_ref=q.at[:, pl.ds(pl.multiple_of((j * NH + h) * cw, cw), cw)],
            send_sem=hs.at[h, r], recv_sem=hr.at[h, nm - r],
            device_id=at(i, d), device_id_type=MESH)

    def hrecv(h, r):
        d = lax.rem(j + r, nm)
        return pltpu.make_async_remote_copy(
            src_ref=qb.at[h, pl.ds(0, bl), :],
            dst_ref=q.at[:, pl.ds(pl.multiple_of((d * NH + h) * cw, cw), cw)],
            send_sem=hs.at[h, r], recv_sem=hr.at[h, r],
            device_id=at(i, d), device_id_type=MESH)

    def hself(h):
        return pltpu.make_async_copy(
            qb.at[h, pl.ds(pl.multiple_of(j * bl, bl), bl), :],
            q.at[:, pl.ds(pl.multiple_of((j * NH + h) * cw, cw), cw)], ls.at[h])

    xcopy(0, 0).wait()
    for h in range(NH):
        wcopy(h).wait()
        qsend[h] = jnp.dot(xv[0, :be, :], wqv[h], preferred_element_type=jnp.float32)
        scopy(h).start()
    xcopy(1, 0).wait()
    for h in range(NH):
        qown[h] = jnp.dot(xv[0, be:, :], wqv[h], preferred_element_type=jnp.float32)

    xcopy(0, 1).wait()
    xcopy(1, 1).wait()
    for n in range(2):
        for r in range(2):
            kcopy(n, r).wait()
    for n, out in ((0, k_out), (1, v_out)):
        for a in range(2):
            acc = jnp.dot(xv[0, a * be:(a + 1) * be, :], wkv[n, 0], preferred_element_type=jnp.float32)
            acc += jnp.dot(xv[1, a * be:(a + 1) * be, :], wkv[n, 1], preferred_element_type=jnp.float32)
            out[pl.ds(pl.multiple_of((ie if a == 0 else i) * be, be), be), :] = acc.astype(jnp.bfloat16)

    for h in range(NH):
        scopy(h).wait_recv()
        qb[h] = (qown[h] + qrecv[h]).astype(jnp.bfloat16)
        for r in (2, 3, 1):
            hcopy(h, r).start()
        hself(h).start()
    for h in range(NH):
        scopy(h).wait_send()
        hself(h).wait()
        for r in range(1, nm):
            hcopy(h, r).wait_send()
            hrecv(h, r).wait_recv()


def _project_in(x, Wq, Wk, Wv, ne, nm):
    b, d = x.shape
    de, hw = Wq.shape
    dh = Wk.shape[1]
    be = b // ne
    bl = be // nm
    cw = hw // NH
    bf, f32 = jnp.bfloat16, jnp.float32
    dma = pltpu.SemaphoreType.DMA
    return pl.pallas_call(
        functools.partial(_in_kernel, ne, nm),
        out_shape=(jax.ShapeDtypeStruct((bl, hw * nm), bf), jax.ShapeDtypeStruct((b, dh), bf),
                   jax.ShapeDtypeStruct((b, dh), bf)),
        in_specs=[_any()] * 4,
        out_specs=(_any(), _vmem(), _vmem()),
        scratch_shapes=[
            pltpu.VMEM((2, b, de), bf), pltpu.VMEM((NH, de, cw), bf), pltpu.VMEM((2, 2, de, dh), bf),
            pltpu.VMEM((NH, be, cw), f32), pltpu.VMEM((NH, be, cw), f32), pltpu.VMEM((NH, be, cw), f32),
            pltpu.VMEM((NH, be, cw), bf),
            dma((2, 2)), dma((NH,)), dma((2, 2)), dma((NH,)), dma((NH,)), dma((NH, nm)), dma((NH, nm)), dma((NH,)),
        ],
        compiler_params=pltpu.CompilerParams(collective_id=0, has_side_effects=True, vmem_limit_bytes=60 << 20),
        name="project_in",
    )(x, Wq, Wk, Wv)


def solution(mesh):
    ne = mesh.shape['emb']
    nm = mesh.shape['model']

    def local(x, Wq, Wk, Wv, Wo, Kc, Vc, lengths):
        q, k_new, v_new = _project_in(x, Wq, Wk, Wv, ne, nm)
        o, k_new, v_new = _attend(q, k_new, v_new, Kc, Vc, lengths, nm)
        y = _project_out(o, Wo, x, ne, nm)
        return y, k_new, v_new

    in_specs = (P('rep', None), P('emb', 'model'), P(), P(), P('model', 'emb'),
                P('rep', None, None), P('rep', None, None), P('rep'))
    out_specs = (P('rep', None), P('rep', None), P('rep', None))
    return jax.shard_map(local, mesh=mesh, in_specs=in_specs, out_specs=out_specs, check_vma=False)
```

```python
import functools

import jax
import jax.numpy as jnp
from jax import lax
from jax.experimental import pallas as pl
from jax.experimental.pallas import tpu as pltpu
from jax.sharding import PartitionSpec as P

MESH = pl.DeviceIdType.MESH
BK = 512
HOOK = 3
VLIM = 60
RING = 6
CH = 4
SUB = 4
NH = 8


def _vmem():
    return pl.BlockSpec(memory_space=pltpu.VMEM)


def _hbm():
    return pl.BlockSpec(memory_space=pltpu.HBM)


def _smem():
    return pl.BlockSpec(memory_space=pltpu.SMEM)


def _qa_kernel(ne, nm, scale, lens, x, wq, wk, wv, kc, vc, ob, olast, k_out, v_out,
               xv, wqv, wkv, qsend, qrecv, qown, qc, qin, qa, qb, oa, obh, ost, knf, vnf, kbuf, vbuf,
               sa, sb, ma, mb, na, nb_,
               xsem, wsem, kvsem, ss0, sr0, ss, sr, hs, hr, osend, orecv, vsend, vrecv, ksem, vsem):
    i = lax.axis_index("emb")
    j = lax.axis_index("model")
    ie = 1 - i
    de = wq.shape[0]
    be = xv.shape[1] // 2
    bl = be // nm
    rows = bl // CH
    kk = wq.shape[1]
    cw = kk // NH
    dh = wk.shape[1]
    nh = ost.shape[2] // dh
    slots = kc.shape[1]
    start = i * be + j * bl

    def at(a, b):
        return {"emb": a, "model": b}

    def xcopy(a, r):
        row = pl.multiple_of((ie if a == 0 else i) * be, be)
        col = pl.multiple_of((i if r == 0 else ie) * de, de)
        return pltpu.make_async_copy(x.at[pl.ds(row, be), pl.ds(col, de)], xv.at[r, a * be:(a + 1) * be, :], xsem.at[a, r])

    def wcopy(h):
        return pltpu.make_async_copy(wq.at[:, pl.ds(h * cw, cw)], wqv.at[h], wsem.at[h])

    def kvcopy(n, r):
        src = wk if n == 0 else wv
        row = pl.multiple_of((i if r == 0 else ie) * de, de)
        return pltpu.make_async_copy(src.at[pl.ds(row, de), :], wkv.at[n, r], kvsem.at[n, r])

    def kcopy(n):
        slot = lax.rem(n, RING)
        return pltpu.make_async_copy(kc.at[start + n], kbuf.at[slot], ksem.at[slot])

    def vcopy(n):
        slot = lax.rem(n, RING)
        return pltpu.make_async_copy(vc.at[start + n], vbuf.at[slot], vsem.at[slot])

    xcopy(0, 0).start()
    for h in range(NH):
        wcopy(h).start()
    xcopy(1, 0).start()
    xcopy(0, 1).start()
    xcopy(1, 1).start()
    for n in range(2):
        for r in range(2):
            kvcopy(n, r).start()
    for n in range(RING - 1):
        kcopy(n).start()
        if n < RING - 2:
            vcopy(n).start()

    barrier = pltpu.get_barrier_semaphore()
    pl.semaphore_signal(barrier, inc=1, device_id=at(ie, j), device_id_type=MESH)
    for r in range(1, nm):
        pl.semaphore_signal(barrier, inc=1, device_id=at(i, lax.rem(j + r, nm)), device_id_type=MESH)
    pl.semaphore_wait(barrier, nm)

    def first(h):
        return pltpu.make_async_remote_copy(
            src_ref=qsend.at[0, :, pl.ds(h * cw, cw)], dst_ref=qrecv.at[0, :, pl.ds(h * cw, cw)],
            send_sem=ss0.at[h], recv_sem=sr0.at[h], device_id=at(ie, j), device_id_type=MESH)

    def later(s):
        return pltpu.make_async_remote_copy(
            src_ref=qsend.at[s], dst_ref=qrecv.at[s], send_sem=ss.at[s], recv_sem=sr.at[s],
            device_id=at(ie, j), device_id_type=MESH)

    def mycols(d):
        return pl.ds(pl.multiple_of(d * kk, kk), kk)

    def hcopy(s, r):
        d = lax.rem(j + r, nm)
        return pltpu.make_async_remote_copy(
            src_ref=qc.at[s, pl.ds(pl.multiple_of(d * rows, rows), rows), :], dst_ref=qin.at[s, :, mycols(j)],
            send_sem=hs.at[s, r], recv_sem=hr.at[s, nm - r], device_id=at(i, d), device_id_type=MESH)

    def hrecv(s, r):
        d = lax.rem(j + r, nm)
        return pltpu.make_async_remote_copy(
            src_ref=qc.at[s, pl.ds(0, rows), :], dst_ref=qin.at[s, :, mycols(d)],
            send_sem=hs.at[s, r], recv_sem=hr.at[s, r], device_id=at(i, d), device_id_type=MESH)

    def block(a, d):
        return pl.ds(pl.multiple_of((a * nm + d) * rows, rows), rows)

    def ocopy(s, r):
        d = lax.rem(j + r, nm)
        return pltpu.make_async_remote_copy(
            src_ref=ost.at[s, :, mycols(d)], dst_ref=ob.at[s, block(i, j), :],
            send_sem=osend.at[s, r], recv_sem=orecv.at[s, nm - r], device_id=at(i, d), device_id_type=MESH)

    def orecv_copy(s, r):
        d = lax.rem(j + r, nm)
        return pltpu.make_async_remote_copy(
            src_ref=ob.at[s, block(i, d), :], dst_ref=ob.at[s, block(i, d), :],
            send_sem=osend.at[s, r], recv_sem=orecv.at[s, r], device_id=at(i, d), device_id_type=MESH)

    def ycopy(s, r):
        dst = ob.at[s, block(i, lax.rem(j + r, nm)), :]
        return pltpu.make_async_remote_copy(
            src_ref=ost.at[s, :, mycols(j)] if r == 0 else dst, dst_ref=dst,
            send_sem=vsend.at[s, r], recv_sem=vrecv.at[s, r], device_id=at(ie, j), device_id_type=MESH)

    def yrecv_copy(s, r):
        blk = ob.at[s, block(ie, lax.rem(j + r, nm)), :]
        return pltpu.make_async_remote_copy(
            src_ref=blk, dst_ref=blk, send_sem=vsend.at[s, r], recv_sem=vrecv.at[s, r],
            device_id=at(ie, j), device_id_type=MESH)

    def spread(dst, h, val):
        for s in range(CH):
            for d in range(nm):
                dst[s, d * rows:(d + 1) * rows, h * cw:(h + 1) * cw] = val[d * bl + s * rows:d * bl + (s + 1) * rows]

    xcopy(0, 0).wait()
    for h in range(NH):
        wcopy(h).wait()
        spread(qsend, h, jnp.dot(xv[0, :be, :], wqv[h], preferred_element_type=jnp.float32))
        first(h).start()
    for s in range(1, CH):
        later(s).start()
    xcopy(1, 0).wait()
    for h in range(NH):
        spread(qown, h, jnp.dot(xv[0, be:, :], wqv[h], preferred_element_type=jnp.float32))
    xcopy(0, 1).wait()
    xcopy(1, 1).wait()
    for n in range(2):
        for r in range(2):
            kvcopy(n, r).wait()
    for n, out, rowf in ((0, k_out, knf), (1, v_out, vnf)):
        for a in range(2):
            acc = jnp.dot(xv[0, a * be:(a + 1) * be, :], wkv[n, 0], preferred_element_type=jnp.float32)
            acc += jnp.dot(xv[1, a * be:(a + 1) * be, :], wkv[n, 1], preferred_element_type=jnp.float32)
            out[pl.ds(pl.multiple_of((ie if a == 0 else i) * be, be), be), :] = acc.astype(jnp.bfloat16)
        rowf[...] = out[pl.ds(pl.multiple_of(start, bl), bl), :].astype(jnp.float32)

    def deal(s):
        qc[s] = (qown[s] + qrecv[s]).astype(jnp.bfloat16)
        for r in (2, 3, 1):
            hcopy(s, r).start()
        qin[s, :, mycols(j)] = qc[s, pl.ds(pl.multiple_of(j * rows, rows), rows), :]

    def relay(s):
        for r in range(1, nm):
            orecv_copy(s, r).wait_recv()
            ycopy(s, r).start()

    for h in range(NH):
        first(h).wait_recv()
    deal(0)

    def scores(s, n, sref, mref, nref):
        t = n - s * rows
        seq = pl.ds(pl.multiple_of(t * nh, nh), nh)
        qf = jnp.concatenate([qa[seq, :], qb[seq, :]], 1)
        q = qf.astype(jnp.bfloat16)
        slot = lax.rem(n, RING)
        new = jnp.sum(qf * knf[pl.ds(n, 1), :], axis=1, keepdims=True) * scale
        count = lens[start + n]
        top = None
        for b in range(slots // BK):
            v = lax.dot_general(q, kbuf[slot, b * BK:(b + 1) * BK, :], (((1,), (1,)), ((), ())),
                                preferred_element_type=jnp.float32) * scale
            v = jnp.where(lax.broadcasted_iota(jnp.int32, v.shape, 1) + b * BK < count, v, -jnp.inf)
            sref[:, b * BK:(b + 1) * BK] = v
            top = v if top is None else jnp.maximum(top, v)
        m = jnp.maximum(jnp.max(top, axis=1, keepdims=True), new)
        mref[...] = jnp.broadcast_to(m, mref.shape)
        nref[...] = jnp.broadcast_to(new, nref.shape)

    def values(s, n, sref, mref, nref):
        t = n - s * rows
        seq = pl.ds(pl.multiple_of(t * nh, nh), nh)
        slot = lax.rem(n, RING)
        m = mref[...]
        wide = jnp.concatenate([m] * (BK // 128), 1)
        ps, tot = [], None
        for b in range(slots // BK):
            p = jnp.exp(sref[:, b * BK:(b + 1) * BK] - wide)
            tot = p if tot is None else tot + p
            ps.append(p.astype(jnp.bfloat16))
        acc = jnp.dot(jnp.concatenate(ps, 1), vbuf[slot], preferred_element_type=jnp.float32)
        pn = jnp.exp(nref[...] - m)
        inv = 1.0 / (jnp.sum(tot, axis=1, keepdims=True) + pn)
        pn = pn.astype(jnp.bfloat16).astype(jnp.float32)
        vn = vnf[pl.ds(n, 1), :]
        oa[seq, :] = (acc[:, :128] + pn * vn[:, :128]) * inv
        obh[seq, :] = (acc[:, 128:] + pn * vn[:, 128:]) * inv

    A, B = (sa, ma, na), (sb, mb, nb_)

    def fetch(n):
        @pl.when(n + RING - 1 < bl)
        def _():
            kcopy(n + RING - 1).start()
            vcopy(n + RING - 2).start()

        @pl.when(n + RING - 1 == bl)
        def _():
            vcopy(n + RING - 2).start()

        @pl.when(n + RING < bl)
        def _():
            kcopy(n + RING).start()
            vcopy(n + RING - 1).start()

        @pl.when(n + RING == bl)
        def _():
            vcopy(n + RING - 1).start()

    def chunk(s, carry):
        n0 = s * rows
        for r in range(1, nm):
            hrecv(s, r).wait_recv()
        for h in range(nh):
            qa[pl.ds(h, rows, stride=nh), :] = qin[s, :, h * dh:h * dh + 128].astype(jnp.float32)
            qb[pl.ds(h, rows, stride=nh), :] = qin[s, :, h * dh + 128:(h + 1) * dh].astype(jnp.float32)
        kcopy(n0).wait()
        scores(s, n0, *A)

        def pair(t, c):
            n = n0 + 2 * t

            @pl.when(t == HOOK)
            def _():
                @pl.when(s + 1 < CH)
                def _():
                    later(s + 1).wait_recv()
                    deal(s + 1)

                @pl.when(s >= 1)
                def _():
                    relay(s - 1)

            fetch(n)
            kcopy(n + 1).wait()
            vcopy(n).wait()
            values(s, n, *A)
            scores(s, n + 1, *B)
            kcopy(n + 2).wait()
            vcopy(n + 1).wait()
            values(s, n + 1, *B)
            scores(s, n + 2, *A)
            return c

        lax.fori_loop(0, rows // 2 - 1, pair, 0)
        n = n0 + rows - 2
        fetch(n)
        kcopy(n + 1).wait()
        vcopy(n).wait()
        values(s, n, *A)
        scores(s, n + 1, *B)
        vcopy(n + 1).wait()
        values(s, n + 1, *B)
        for h in range(nh):
            ost[s, :, h * dh:h * dh + 128] = oa[pl.ds(h, rows, stride=nh), :].astype(jnp.bfloat16)
            ost[s, :, h * dh + 128:(h + 1) * dh] = obh[pl.ds(h, rows, stride=nh), :].astype(jnp.bfloat16)

        @pl.when(s < CH - 1)
        def _():
            for r in (2, 3, 1):
                ocopy(s, r).start()
            ycopy(s, 0).start()
            ob[s, block(i, j), :] = ost[s, :, mycols(j)]

        return carry

    lax.fori_loop(0, CH, chunk, 0)
    olast[...] = ost[CH - 1]
    for h in range(NH):
        first(h).wait_send()
    for s in range(CH):
        if s:
            later(s).wait_send()
        for r in range(1, nm):
            hcopy(s, r).wait_send()
            if s < CH - 1:
                ocopy(s, r).wait_send()
        if s < CH - 1:
            for r in range(nm):
                ycopy(s, r).wait_send()
                yrecv_copy(s, r).wait_recv()


def _attend(x, Wq, Wk, Wv, Kc, Vc, lengths, ne, nm):
    b, d = x.shape
    de, kk = Wq.shape
    dh = Wk.shape[1]
    slots = Kc.shape[1]
    be = b // ne
    bl = be // nm
    rows = bl // CH
    cw = kk // NH
    full = kk * nm
    nh = full // dh
    assert dh == 256 and slots % BK == 0
    bf, f32 = jnp.bfloat16, jnp.float32
    dma = pltpu.SemaphoreType.DMA
    V = pltpu.VMEM
    part = V((CH, nm * rows, kk), f32)
    flat = V((rows * nh, 128), f32)
    stat = V((nh, 128), f32)
    return pl.pallas_call(
        functools.partial(_qa_kernel, ne, nm, dh ** -0.5),
        out_shape=(V((CH - 1, b // CH, kk), bf), V((rows, full), bf), V((b, dh), bf), V((b, dh), bf)),
        in_specs=[_smem()] + [_hbm()] * 6,
        out_specs=(_vmem(),) * 4,
        scratch_shapes=[
            V((2, b, de), bf), V((NH, de, cw), bf), V((2, 2, de, dh), bf), part, part, part,
            V((CH, nm * rows, kk), bf), V((CH, rows, full), bf), flat, flat, flat, flat, V((CH, rows, full), bf),
            V((bl, dh), f32), V((bl, dh), f32), V((RING, slots, dh), bf), V((RING, slots, dh), bf),
            V((nh, slots), f32), V((nh, slots), f32), stat, stat, stat, stat,
            dma((2, 2)), dma((NH,)), dma((2, 2)), dma((NH,)), dma((NH,)), dma((CH,)), dma((CH,)),
            dma((CH, nm)), dma((CH, nm)), dma((CH, nm)), dma((CH, nm)), dma((CH, nm)), dma((CH, nm)),
            dma((RING,)), dma((RING,)),
        ],
        compiler_params=pltpu.CompilerParams(collective_id=0, has_side_effects=True, vmem_limit_bytes=VLIM << 20),
        name="attend",
    )(lengths, x, Wq, Wk, Wv, Kc, Vc)


def _out_kernel(ne, nm, od_ref, o_ref, wo, x, y, wv, xv, ob, pown, psend, precv, ssend, srecv,
                wsem, xsem, osend, orecv, vsend, vrecv, ps, pr, xs_, xr, cs, cr, es, er, fs, fr):
    i = lax.axis_index("emb")
    j = lax.axis_index("model")
    c = lax.rem(j, 2)
    jp = j + 1 - 2 * c
    jx = lax.rem(j + 2, nm)
    ie = 1 - i
    half = wv.shape[2]
    cw = half // SUB
    rows = o_ref.shape[0]
    kk = wv.shape[1]
    dev = ne * nm

    def at(a, b):
        return {"emb": a, "model": b}

    def wcopy(b, u):
        col = pl.multiple_of((1 - c if b == 0 else c) * half + u * cw, cw)
        return pltpu.make_async_copy(wo.at[:, pl.ds(col, cw)], wv.at[b, :, pl.ds(u * cw, cw)], wsem.at[b, u])

    for b in range(2):
        for u in range(SUB):
            wcopy(b, u).start()
    mycol = pl.multiple_of((i * 2 + c) * half, half)
    excol = pl.multiple_of((ie * 2 + c) * half, half)
    xcopy = pltpu.make_async_copy(x.at[:, :, pl.ds(mycol, half)], xv, xsem)
    xcopy.start()

    barrier = pltpu.get_barrier_semaphore()
    pl.semaphore_signal(barrier, inc=1, device_id=at(ie, j), device_id_type=MESH)
    for r in range(1, nm):
        pl.semaphore_signal(barrier, inc=1, device_id=at(i, lax.rem(j + r, nm)), device_id_type=MESH)
    pl.semaphore_wait(barrier, nm)

    def block(a, d):
        return pl.ds(pl.multiple_of((a * nm + d) * rows, rows), rows)

    def heads(d):
        return pl.ds(pl.multiple_of(d * kk, kk), kk)

    def ocopy(r):
        d = lax.rem(j + r, nm)
        return pltpu.make_async_remote_copy(
            src_ref=o_ref.at[:, heads(d)], dst_ref=ob.at[block(i, j), :],
            send_sem=osend.at[r], recv_sem=orecv.at[nm - r], device_id=at(i, d), device_id_type=MESH)

    def orecv_copy(r):
        d = lax.rem(j + r, nm)
        return pltpu.make_async_remote_copy(
            src_ref=ob.at[block(i, d), :], dst_ref=ob.at[block(i, d), :],
            send_sem=osend.at[r], recv_sem=orecv.at[r], device_id=at(i, d), device_id_type=MESH)

    def vcopy(r):
        dst = ob.at[block(i, lax.rem(j + r, nm)), :]
        return pltpu.make_async_remote_copy(
            src_ref=o_ref.at[:, heads(j)] if r == 0 else dst, dst_ref=dst,
            send_sem=vsend.at[r], recv_sem=vrecv.at[r], device_id=at(ie, j), device_id_type=MESH)

    def vrecv_copy(r):
        blk = ob.at[block(ie, lax.rem(j + r, nm)), :]
        return pltpu.make_async_remote_copy(
            src_ref=blk, dst_ref=blk, send_sem=vsend.at[r], recv_sem=vrecv.at[r],
            device_id=at(ie, j), device_id_type=MESH)

    for r in (2, 3, 1):
        ocopy(r).start()
    vcopy(0).start()
    ob[block(i, j), :] = o_ref[:, heads(j)]

    def pcopy(s, u):
        return pltpu.make_async_remote_copy(
            src_ref=psend.at[s, u], dst_ref=precv.at[s, u], send_sem=ps.at[s, u], recv_sem=pr.at[s, u],
            device_id=at(i, jp), device_id_type=MESH)

    def scopy(s, u):
        return pltpu.make_async_remote_copy(
            src_ref=ssend.at[s, u], dst_ref=srecv.at[s, u], send_sem=xs_.at[s, u], recv_sem=xr.at[s, u],
            device_id=at(i, jx), device_id_type=MESH)

    def piece(s, u, base):
        return y.at[:, pl.ds(pl.multiple_of(s * rows, rows), rows), pl.ds(pl.multiple_of(base + u * cw, cw), cw)]

    def ccopy(s, u):
        return pltpu.make_async_remote_copy(
            src_ref=piece(s, u, mycol), dst_ref=piece(s, u, mycol), send_sem=cs.at[s, u], recv_sem=cr.at[s, u],
            device_id=at(i, jp), device_id_type=MESH)

    def ecopy(s, u):
        return pltpu.make_async_remote_copy(
            src_ref=piece(s, u, mycol), dst_ref=piece(s, u, mycol), send_sem=es.at[s, u], recv_sem=er.at[s, u],
            device_id=at(ie, j), device_id_type=MESH)

    def fcopy(s, u):
        return pltpu.make_async_remote_copy(
            src_ref=piece(s, u, excol), dst_ref=piece(s, u, excol), send_sem=fs.at[s, u], recv_sem=fr.at[s, u],
            device_id=at(i, jp), device_id_type=MESH)

    def compute(s, lhs):
        for u in range(SUB):
            @pl.when(s == 0)
            def _():
                wcopy(0, u).wait()

            psend[s, u] = jnp.dot(lhs(), wv[0, :, u * cw:(u + 1) * cw],
                                  preferred_element_type=jnp.float32).astype(jnp.bfloat16)
            pcopy(s, u).start()
        for u in range(SUB):
            @pl.when(s == 0)
            def _():
                wcopy(1, u).wait()

            pown[u] = jnp.dot(lhs(), wv[1, :, u * cw:(u + 1) * cw], preferred_element_type=jnp.float32)
            pcopy(s, u).wait_recv()
            ssend[s, u] = (pown[u] + precv[s, u].astype(jnp.float32)).astype(jnp.bfloat16)
            scopy(s, u).start()

    def finish(s):
        at_rows = pl.ds(pl.multiple_of(s * rows, rows), rows)
        for u in range(SUB):
            scopy(s, u).wait_recv()
            tot = ssend[s, u].astype(jnp.float32) + srecv[s, u].astype(jnp.float32)
            xs = xv[:, at_rows, u * cw:(u + 1) * cw].astype(jnp.float32)
            y[:, at_rows, pl.ds(pl.multiple_of(mycol + u * cw, cw), cw)] = (
                xs + tot.reshape(dev, rows, cw)).astype(jnp.bfloat16)
            ecopy(s, u).start()
            ccopy(s, u).start()

    def forward(s):
        for u in range(SUB):
            ecopy(s, u).wait_recv()
            fcopy(s, u).start()

    def step(s, carry):
        compute(s, lambda: od_ref[s])

        @pl.when(s == 0)
        def _():
            for r in range(1, nm):
                orecv_copy(r).wait_recv()
                vcopy(r).start()
            xcopy.wait()

        @pl.when(s >= 1)
        def _():
            finish(s - 1)

        @pl.when(s >= 2)
        def _():
            forward(s - 2)

        return carry

    lax.fori_loop(0, CH - 1, step, 0)
    for r in range(nm):
        vrecv_copy(r).wait_recv()
    compute(CH - 1, lambda: ob[...])
    finish(CH - 2)
    forward(CH - 3)
    finish(CH - 1)
    forward(CH - 2)
    forward(CH - 1)
    for r in range(1, nm):
        ocopy(r).wait_send()
    for r in range(nm):
        vcopy(r).wait_send()
    for s in range(CH):
        for u in range(SUB):
            pcopy(s, u).wait_send()
            scopy(s, u).wait_send()
            ecopy(s, u).wait_send()
            ccopy(s, u).wait()
            fcopy(s, u).wait()


def _project_out(done, last, Wo, x, ne, nm):
    bl = CH * last.shape[0]
    kk, ncol = Wo.shape
    half = ncol // 2
    dev = ne * nm
    rows = bl // CH
    cw = half // SUB
    b, d = x.shape
    bf, f32 = jnp.bfloat16, jnp.float32
    dma = pltpu.SemaphoreType.DMA
    pieces = pltpu.VMEM((CH, SUB, dev * rows, cw), bf)
    y = pl.pallas_call(
        functools.partial(_out_kernel, ne, nm),
        out_shape=pltpu.VMEM((dev, bl, d), bf),
        in_specs=[_vmem(), _vmem(), _hbm(), _hbm()],
        out_specs=_vmem(),
        scratch_shapes=[
            pltpu.VMEM((2, kk, half), bf), pltpu.VMEM((dev, bl, half), bf), pltpu.VMEM((dev * rows, kk), bf),
            pltpu.VMEM((SUB, dev * rows, cw), f32), pieces, pieces, pieces, pieces,
            dma((2, SUB)), dma,
        ] + [dma((nm,))] * 4 + [dma((CH, SUB))] * 10,
        compiler_params=pltpu.CompilerParams(collective_id=1, has_side_effects=True, vmem_limit_bytes=36 << 20),
        name="project_out",
    )(done, last, Wo, x.reshape(dev, bl, d))
    return y.reshape(b, d)


def solution(mesh):
    ne = mesh.shape['emb']
    nm = mesh.shape['model']

    def local(x, Wq, Wk, Wv, Wo, Kc, Vc, lengths):
        done, last, k_new, v_new = _attend(x, Wq, Wk, Wv, Kc, Vc, lengths, ne, nm)
        y = _project_out(done, last, Wo, x, ne, nm)
        return y, k_new, v_new

    in_specs = (P('rep', None), P('emb', 'model'), P(), P(), P('model', 'emb'),
                P('rep', None, None), P('rep', None, None), P('rep'))
    out_specs = (P('rep', None), P('rep', None), P('rep', None))
    return jax.shard_map(local, mesh=mesh, in_specs=in_specs, out_specs=out_specs, check_vma=False)
```

```python
import functools

import jax
import jax.numpy as jnp
from jax import lax
from jax.experimental import pallas as pl
from jax.experimental.pallas import tpu as pltpu
from jax.sharding import PartitionSpec as P

MESH = pl.DeviceIdType.MESH
BK = 512
VLIM = 60
DEAL = 1
RELAY = 2
RING = 6
CH = 8
SUB = 4
NH = 8


def _vmem():
    return pl.BlockSpec(memory_space=pltpu.VMEM)


def _hbm():
    return pl.BlockSpec(memory_space=pltpu.HBM)


def _smem():
    return pl.BlockSpec(memory_space=pltpu.SMEM)


def _qa_kernel(ne, nm, scale, lens, x, wq, wk, wv, kc, vc, ob, olast, k_out, v_out,
               xv, wqv, wkv, qsend, qrecv, qown, qc, qin, qa, qb, oa, obh, ost, knf, vnf, kbuf, vbuf,
               sa, sb, ma, mb, na, nb_,
               xsem, wsem, kvsem, ss0, sr0, ss, sr, hs, hr, osend, orecv, vsend, vrecv, ksem, vsem):
    i = lax.axis_index("emb")
    j = lax.axis_index("model")
    ie = 1 - i
    de = wq.shape[0]
    be = xv.shape[1] // 2
    bl = be // nm
    rows = bl // CH
    kk = wq.shape[1]
    cw = kk // NH
    dh = wk.shape[1]
    nh = ost.shape[2] // dh
    slots = kc.shape[1]
    start = i * be + j * bl

    def at(a, b):
        return {"emb": a, "model": b}

    def xcopy(a, r):
        row = pl.multiple_of((ie if a == 0 else i) * be, be)
        col = pl.multiple_of((i if r == 0 else ie) * de, de)
        return pltpu.make_async_copy(x.at[pl.ds(row, be), pl.ds(col, de)], xv.at[r, a * be:(a + 1) * be, :], xsem.at[a, r])

    def wcopy(h):
        return pltpu.make_async_copy(wq.at[:, pl.ds(h * cw, cw)], wqv.at[h], wsem.at[h])

    def kvcopy(n, r):
        src = wk if n == 0 else wv
        row = pl.multiple_of((i if r == 0 else ie) * de, de)
        return pltpu.make_async_copy(src.at[pl.ds(row, de), :], wkv.at[n, r], kvsem.at[n, r])

    def kcopy(n):
        slot = lax.rem(n, RING)
        return pltpu.make_async_copy(kc.at[start + n], kbuf.at[slot], ksem.at[slot])

    def vcopy(n):
        slot = lax.rem(n, RING)
        return pltpu.make_async_copy(vc.at[start + n], vbuf.at[slot], vsem.at[slot])

    xcopy(0, 0).start()
    for h in range(NH):
        wcopy(h).start()
    xcopy(1, 0).start()
    xcopy(0, 1).start()
    xcopy(1, 1).start()
    for n in range(2):
        for r in range(2):
            kvcopy(n, r).start()
    for n in range(RING - 1):
        kcopy(n).start()
        if n < RING - 2:
            vcopy(n).start()

    barrier = pltpu.get_barrier_semaphore()
    pl.semaphore_signal(barrier, inc=1, device_id=at(ie, j), device_id_type=MESH)
    for r in range(1, nm):
        pl.semaphore_signal(barrier, inc=1, device_id=at(i, lax.rem(j + r, nm)), device_id_type=MESH)
    pl.semaphore_wait(barrier, nm)

    def first(h):
        return pltpu.make_async_remote_copy(
            src_ref=qsend.at[0, :, pl.ds(h * cw, cw)], dst_ref=qrecv.at[0, :, pl.ds(h * cw, cw)],
            send_sem=ss0.at[h], recv_sem=sr0.at[h], device_id=at(ie, j), device_id_type=MESH)

    def later(s):
        return pltpu.make_async_remote_copy(
            src_ref=qsend.at[s], dst_ref=qrecv.at[s], send_sem=ss.at[s], recv_sem=sr.at[s],
            device_id=at(ie, j), device_id_type=MESH)

    def mycols(d):
        return pl.ds(pl.multiple_of(d * kk, kk), kk)

    def hcopy(s, r):
        d = lax.rem(j + r, nm)
        return pltpu.make_async_remote_copy(
            src_ref=qc.at[s, pl.ds(pl.multiple_of(d * rows, rows), rows), :], dst_ref=qin.at[s, :, mycols(j)],
            send_sem=hs.at[s, r], recv_sem=hr.at[s, nm - r], device_id=at(i, d), device_id_type=MESH)

    def hrecv(s, r):
        d = lax.rem(j + r, nm)
        return pltpu.make_async_remote_copy(
            src_ref=qc.at[s, pl.ds(0, rows), :], dst_ref=qin.at[s, :, mycols(d)],
            send_sem=hs.at[s, r], recv_sem=hr.at[s, r], device_id=at(i, d), device_id_type=MESH)

    def block(a, d):
        return pl.ds(pl.multiple_of((a * nm + d) * rows, rows), rows)

    def ocopy(s, r):
        d = lax.rem(j + r, nm)
        return pltpu.make_async_remote_copy(
            src_ref=ost.at[s, :, mycols(d)], dst_ref=ob.at[s, block(i, j), :],
            send_sem=osend.at[s, r], recv_sem=orecv.at[s, nm - r], device_id=at(i, d), device_id_type=MESH)

    def orecv_copy(s, r):
        d = lax.rem(j + r, nm)
        return pltpu.make_async_remote_copy(
            src_ref=ob.at[s, block(i, d), :], dst_ref=ob.at[s, block(i, d), :],
            send_sem=osend.at[s, r], recv_sem=orecv.at[s, r], device_id=at(i, d), device_id_type=MESH)

    def ycopy(s, r):
        dst = ob.at[s, block(i, lax.rem(j + r, nm)), :]
        return pltpu.make_async_remote_copy(
            src_ref=ost.at[s, :, mycols(j)] if r == 0 else dst, dst_ref=dst,
            send_sem=vsend.at[s, r], recv_sem=vrecv.at[s, r], device_id=at(ie, j), device_id_type=MESH)

    def yrecv_copy(s, r):
        blk = ob.at[s, block(ie, lax.rem(j + r, nm)), :]
        return pltpu.make_async_remote_copy(
            src_ref=blk, dst_ref=blk, send_sem=vsend.at[s, r], recv_sem=vrecv.at[s, r],
            device_id=at(ie, j), device_id_type=MESH)

    def spread(dst, h, val):
        for s in range(CH):
            for d in range(nm):
                dst[s, d * rows:(d + 1) * rows, h * cw:(h + 1) * cw] = val[d * bl + s * rows:d * bl + (s + 1) * rows]

    xcopy(0, 0).wait()
    for h in range(NH):
        wcopy(h).wait()
        spread(qsend, h, jnp.dot(xv[0, :be, :], wqv[h], preferred_element_type=jnp.float32))
        first(h).start()
    for s in range(1, CH):
        later(s).start()
    xcopy(1, 0).wait()
    for h in range(NH):
        spread(qown, h, jnp.dot(xv[0, be:, :], wqv[h], preferred_element_type=jnp.float32))
    def deal(s):
        qc[s] = (qown[s] + qrecv[s]).astype(jnp.bfloat16)
        for r in (2, 3, 1):
            hcopy(s, r).start()
        qin[s, :, mycols(j)] = qc[s, pl.ds(pl.multiple_of(j * rows, rows), rows), :]

    def relay(s):
        for r in range(1, nm):
            orecv_copy(s, r).wait_recv()
            ycopy(s, r).start()

    for h in range(NH):
        first(h).wait_recv()
    deal(0)

    xcopy(0, 1).wait()
    xcopy(1, 1).wait()
    for n in range(2):
        for r in range(2):
            kvcopy(n, r).wait()
    for n, out, rowf in ((0, k_out, knf), (1, v_out, vnf)):
        for a in range(2):
            acc = jnp.dot(xv[0, a * be:(a + 1) * be, :], wkv[n, 0], preferred_element_type=jnp.float32)
            acc += jnp.dot(xv[1, a * be:(a + 1) * be, :], wkv[n, 1], preferred_element_type=jnp.float32)
            out[pl.ds(pl.multiple_of((ie if a == 0 else i) * be, be), be), :] = acc.astype(jnp.bfloat16)
        rowf[...] = out[pl.ds(pl.multiple_of(start, bl), bl), :].astype(jnp.float32)

    def scores(n, sref, mref, nref):
        t = n % rows
        seq = pl.ds(pl.multiple_of(t * nh, nh), nh)
        qf = jnp.concatenate([qa[seq, :], qb[seq, :]], 1)
        q = qf.astype(jnp.bfloat16)
        slot = lax.rem(n, RING)
        new = jnp.sum(qf * knf[pl.ds(n, 1), :], axis=1, keepdims=True) * scale
        count = lens[start + n]
        top = None
        for b in range(slots // BK):
            v = lax.dot_general(q, kbuf[slot, b * BK:(b + 1) * BK, :], (((1,), (1,)), ((), ())),
                                preferred_element_type=jnp.float32) * scale
            v = jnp.where(lax.broadcasted_iota(jnp.int32, v.shape, 1) + b * BK < count, v, -jnp.inf)
            sref[:, b * BK:(b + 1) * BK] = v
            top = v if top is None else jnp.maximum(top, v)
        m = jnp.maximum(jnp.max(top, axis=1, keepdims=True), new)
        mref[...] = jnp.broadcast_to(m, mref.shape)
        nref[...] = jnp.broadcast_to(new, nref.shape)

    def values(n, sref, mref, nref):
        t = n % rows
        seq = pl.ds(pl.multiple_of(t * nh, nh), nh)
        slot = lax.rem(n, RING)
        m = mref[...]
        wide = jnp.concatenate([m] * (BK // 128), 1)
        ps, tot = [], None
        for b in range(slots // BK):
            p = jnp.exp(sref[:, b * BK:(b + 1) * BK] - wide)
            tot = p if tot is None else tot + p
            ps.append(p.astype(jnp.bfloat16))
        acc = jnp.dot(jnp.concatenate(ps, 1), vbuf[slot], preferred_element_type=jnp.float32)
        pn = jnp.exp(nref[...] - m)
        inv = 1.0 / (jnp.sum(tot, axis=1, keepdims=True) + pn)
        pn = pn.astype(jnp.bfloat16).astype(jnp.float32)
        vn = vnf[pl.ds(n, 1), :]
        oa[seq, :] = (acc[:, :128] + pn * vn[:, :128]) * inv
        obh[seq, :] = (acc[:, 128:] + pn * vn[:, 128:]) * inv

    A, B = (sa, ma, na), (sb, mb, nb_)

    def fetch(n):
        @pl.when(n + RING - 1 < bl)
        def _():
            kcopy(n + RING - 1).start()
            vcopy(n + RING - 2).start()

        @pl.when(n + RING - 1 == bl)
        def _():
            vcopy(n + RING - 2).start()

        @pl.when(n + RING < bl)
        def _():
            kcopy(n + RING).start()
            vcopy(n + RING - 1).start()

        @pl.when(n + RING == bl)
        def _():
            vcopy(n + RING - 1).start()

    per = rows // 2

    def load_q(s):
        for r in range(1, nm):
            hrecv(s, r).wait_recv()
        for h in range(nh):
            qa[pl.ds(h, rows, stride=nh), :] = qin[s, :, h * dh:h * dh + 128].astype(jnp.float32)
            qb[pl.ds(h, rows, stride=nh), :] = qin[s, :, h * dh + 128:(h + 1) * dh].astype(jnp.float32)

    def store_o(s):
        for h in range(nh):
            ost[s, :, h * dh:h * dh + 128] = oa[pl.ds(h, rows, stride=nh), :].astype(jnp.bfloat16)
            ost[s, :, h * dh + 128:(h + 1) * dh] = obh[pl.ds(h, rows, stride=nh), :].astype(jnp.bfloat16)

    load_q(0)
    kcopy(0).wait()
    scores(0, *A)

    def pair(p, c):
        n = 2 * p
        s = p // per
        t = p % per

        @pl.when(t == DEAL)
        def _():
            @pl.when(s + 1 < CH)
            def _():
                later(s + 1).wait_recv()
                deal(s + 1)

        @pl.when(t == RELAY)
        def _():
            @pl.when(s >= 1)
            def _():
                relay(s - 1)

        fetch(n)
        kcopy(n + 1).wait()
        vcopy(n).wait()
        values(n, *A)
        scores(n + 1, *B)

        @pl.when(t == per - 1)
        def _():
            load_q(s + 1)

        kcopy(n + 2).wait()
        vcopy(n + 1).wait()
        values(n + 1, *B)
        scores(n + 2, *A)

        @pl.when(t == per - 1)
        def _():
            store_o(s)
            for r in (2, 3, 1):
                ocopy(s, r).start()
            ycopy(s, 0).start()
            ob[s, block(i, j), :] = ost[s, :, mycols(j)]

        return c

    lax.fori_loop(0, bl // 2 - 1, pair, 0)
    kcopy(bl - 1).wait()
    vcopy(bl - 2).wait()
    values(bl - 2, *A)
    scores(bl - 1, *B)
    vcopy(bl - 1).wait()
    values(bl - 1, *B)
    store_o(CH - 1)
    olast[...] = ost[CH - 1]
    for h in range(NH):
        first(h).wait_send()
    for s in range(CH):
        if s:
            later(s).wait_send()
        for r in range(1, nm):
            hcopy(s, r).wait_send()
            if s < CH - 1:
                ocopy(s, r).wait_send()
        if s < CH - 1:
            for r in range(nm):
                ycopy(s, r).wait_send()
                yrecv_copy(s, r).wait_recv()


def _attend(x, Wq, Wk, Wv, Kc, Vc, lengths, ne, nm):
    b, d = x.shape
    de, kk = Wq.shape
    dh = Wk.shape[1]
    slots = Kc.shape[1]
    be = b // ne
    bl = be // nm
    rows = bl // CH
    cw = kk // NH
    full = kk * nm
    nh = full // dh
    assert dh == 256 and slots % BK == 0
    bf, f32 = jnp.bfloat16, jnp.float32
    dma = pltpu.SemaphoreType.DMA
    V = pltpu.VMEM
    part = V((CH, nm * rows, kk), f32)
    flat = V((rows * nh, 128), f32)
    stat = V((nh, 128), f32)
    return pl.pallas_call(
        functools.partial(_qa_kernel, ne, nm, dh ** -0.5),
        out_shape=(V((CH - 1, b // CH, kk), bf), V((rows, full), bf), V((b, dh), bf), V((b, dh), bf)),
        in_specs=[_smem()] + [_hbm()] * 6,
        out_specs=(_vmem(),) * 4,
        scratch_shapes=[
            V((2, b, de), bf), V((NH, de, cw), bf), V((2, 2, de, dh), bf), part, part, part,
            V((CH, nm * rows, kk), bf), V((CH, rows, full), bf), flat, flat, flat, flat, V((CH, rows, full), bf),
            V((bl, dh), f32), V((bl, dh), f32), V((RING, slots, dh), bf), V((RING, slots, dh), bf),
            V((nh, slots), f32), V((nh, slots), f32), stat, stat, stat, stat,
            dma((2, 2)), dma((NH,)), dma((2, 2)), dma((NH,)), dma((NH,)), dma((CH,)), dma((CH,)),
            dma((CH, nm)), dma((CH, nm)), dma((CH, nm)), dma((CH, nm)), dma((CH, nm)), dma((CH, nm)),
            dma((RING,)), dma((RING,)),
        ],
        compiler_params=pltpu.CompilerParams(collective_id=0, has_side_effects=True, vmem_limit_bytes=VLIM << 20),
        name="attend",
    )(lengths, x, Wq, Wk, Wv, Kc, Vc)


def _out_kernel(ne, nm, od_ref, o_ref, wo, x, y, wv, xv, ob, pown, psend, precv, ssend, srecv,
                wsem, xsem, osend, orecv, vsend, vrecv, ps, pr, xs_, xr, cs, cr, es, er, fs, fr):
    i = lax.axis_index("emb")
    j = lax.axis_index("model")
    c = lax.rem(j, 2)
    jp = j + 1 - 2 * c
    jx = lax.rem(j + 2, nm)
    ie = 1 - i
    half = wv.shape[2]
    cw = half // SUB
    rows = o_ref.shape[0]
    kk = wv.shape[1]
    dev = ne * nm

    def at(a, b):
        return {"emb": a, "model": b}

    def wcopy(b, u):
        col = pl.multiple_of((1 - c if b == 0 else c) * half + u * cw, cw)
        return pltpu.make_async_copy(wo.at[:, pl.ds(col, cw)], wv.at[b, :, pl.ds(u * cw, cw)], wsem.at[b, u])

    for b in range(2):
        for u in range(SUB):
            wcopy(b, u).start()
    mycol = pl.multiple_of((i * 2 + c) * half, half)
    excol = pl.multiple_of((ie * 2 + c) * half, half)
    xcopy = pltpu.make_async_copy(x.at[:, :, pl.ds(mycol, half)], xv, xsem)
    xcopy.start()

    barrier = pltpu.get_barrier_semaphore()
    pl.semaphore_signal(barrier, inc=1, device_id=at(ie, j), device_id_type=MESH)
    for r in range(1, nm):
        pl.semaphore_signal(barrier, inc=1, device_id=at(i, lax.rem(j + r, nm)), device_id_type=MESH)
    pl.semaphore_wait(barrier, nm)

    def block(a, d):
        return pl.ds(pl.multiple_of((a * nm + d) * rows, rows), rows)

    def heads(d):
        return pl.ds(pl.multiple_of(d * kk, kk), kk)

    def ocopy(r):
        d = lax.rem(j + r, nm)
        return pltpu.make_async_remote_copy(
            src_ref=o_ref.at[:, heads(d)], dst_ref=ob.at[block(i, j), :],
            send_sem=osend.at[r], recv_sem=orecv.at[nm - r], device_id=at(i, d), device_id_type=MESH)

    def orecv_copy(r):
        d = lax.rem(j + r, nm)
        return pltpu.make_async_remote_copy(
            src_ref=ob.at[block(i, d), :], dst_ref=ob.at[block(i, d), :],
            send_sem=osend.at[r], recv_sem=orecv.at[r], device_id=at(i, d), device_id_type=MESH)

    def vcopy(r):
        dst = ob.at[block(i, lax.rem(j + r, nm)), :]
        return pltpu.make_async_remote_copy(
            src_ref=o_ref.at[:, heads(j)] if r == 0 else dst, dst_ref=dst,
            send_sem=vsend.at[r], recv_sem=vrecv.at[r], device_id=at(ie, j), device_id_type=MESH)

    def vrecv_copy(r):
        blk = ob.at[block(ie, lax.rem(j + r, nm)), :]
        return pltpu.make_async_remote_copy(
            src_ref=blk, dst_ref=blk, send_sem=vsend.at[r], recv_sem=vrecv.at[r],
            device_id=at(ie, j), device_id_type=MESH)

    for r in (2, 3, 1):
        ocopy(r).start()
    vcopy(0).start()
    ob[block(i, j), :] = o_ref[:, heads(j)]

    def pcopy(s, u):
        return pltpu.make_async_remote_copy(
            src_ref=psend.at[s, u], dst_ref=precv.at[s, u], send_sem=ps.at[s, u], recv_sem=pr.at[s, u],
            device_id=at(i, jp), device_id_type=MESH)

    def scopy(s, u):
        return pltpu.make_async_remote_copy(
            src_ref=ssend.at[s, u], dst_ref=srecv.at[s, u], send_sem=xs_.at[s, u], recv_sem=xr.at[s, u],
            device_id=at(i, jx), device_id_type=MESH)

    def piece(s, u, base):
        return y.at[:, pl.ds(pl.multiple_of(s * rows, rows), rows), pl.ds(pl.multiple_of(base + u * cw, cw), cw)]

    def ccopy(s, u):
        return pltpu.make_async_remote_copy(
            src_ref=piece(s, u, mycol), dst_ref=piece(s, u, mycol), send_sem=cs.at[s, u], recv_sem=cr.at[s, u],
            device_id=at(i, jp), device_id_type=MESH)

    def ecopy(s, u):
        return pltpu.make_async_remote_copy(
            src_ref=piece(s, u, mycol), dst_ref=piece(s, u, mycol), send_sem=es.at[s, u], recv_sem=er.at[s, u],
            device_id=at(ie, j), device_id_type=MESH)

    def fcopy(s, u):
        return pltpu.make_async_remote_copy(
            src_ref=piece(s, u, excol), dst_ref=piece(s, u, excol), send_sem=fs.at[s, u], recv_sem=fr.at[s, u],
            device_id=at(i, jp), device_id_type=MESH)

    def compute(s, lhs):
        for u in range(SUB):
            @pl.when(s == 0)
            def _():
                wcopy(0, u).wait()

            psend[s, u] = jnp.dot(lhs(), wv[0, :, u * cw:(u + 1) * cw],
                                  preferred_element_type=jnp.float32).astype(jnp.bfloat16)
            pcopy(s, u).start()
        for u in range(SUB):
            @pl.when(s == 0)
            def _():
                wcopy(1, u).wait()

            pown[u] = jnp.dot(lhs(), wv[1, :, u * cw:(u + 1) * cw], preferred_element_type=jnp.float32)
            pcopy(s, u).wait_recv()
            ssend[s, u] = (pown[u] + precv[s, u].astype(jnp.float32)).astype(jnp.bfloat16)
            scopy(s, u).start()

    def finish(s):
        at_rows = pl.ds(pl.multiple_of(s * rows, rows), rows)
        for u in range(SUB):
            scopy(s, u).wait_recv()
            tot = ssend[s, u].astype(jnp.float32) + srecv[s, u].astype(jnp.float32)
            xs = xv[:, at_rows, u * cw:(u + 1) * cw].astype(jnp.float32)
            y[:, at_rows, pl.ds(pl.multiple_of(mycol + u * cw, cw), cw)] = (
                xs + tot.reshape(dev, rows, cw)).astype(jnp.bfloat16)
            ecopy(s, u).start()
            ccopy(s, u).start()

    def forward(s):
        for u in range(SUB):
            ecopy(s, u).wait_recv()
            fcopy(s, u).start()

    def step(s, carry):
        compute(s, lambda: od_ref[s])

        @pl.when(s == 0)
        def _():
            for r in range(1, nm):
                orecv_copy(r).wait_recv()
                vcopy(r).start()
            xcopy.wait()

        @pl.when(s >= 1)
        def _():
            finish(s - 1)

        @pl.when(s >= 2)
        def _():
            forward(s - 2)

        return carry

    lax.fori_loop(0, CH - 1, step, 0)
    for r in range(nm):
        vrecv_copy(r).wait_recv()
    compute(CH - 1, lambda: ob[...])
    finish(CH - 2)
    forward(CH - 3)
    finish(CH - 1)
    forward(CH - 2)
    forward(CH - 1)
    for r in range(1, nm):
        ocopy(r).wait_send()
    for r in range(nm):
        vcopy(r).wait_send()
    for s in range(CH):
        for u in range(SUB):
            pcopy(s, u).wait_send()
            scopy(s, u).wait_send()
            ecopy(s, u).wait_send()
            ccopy(s, u).wait()
            fcopy(s, u).wait()


def _project_out(done, last, Wo, x, ne, nm):
    bl = CH * last.shape[0]
    kk, ncol = Wo.shape
    half = ncol // 2
    dev = ne * nm
    rows = bl // CH
    cw = half // SUB
    b, d = x.shape
    bf, f32 = jnp.bfloat16, jnp.float32
    dma = pltpu.SemaphoreType.DMA
    pieces = pltpu.VMEM((CH, SUB, dev * rows, cw), bf)
    y = pl.pallas_call(
        functools.partial(_out_kernel, ne, nm),
        out_shape=pltpu.VMEM((dev, bl, d), bf),
        in_specs=[_vmem(), _vmem(), _hbm(), _hbm()],
        out_specs=_vmem(),
        scratch_shapes=[
            pltpu.VMEM((2, kk, half), bf), pltpu.VMEM((dev, bl, half), bf), pltpu.VMEM((dev * rows, kk), bf),
            pltpu.VMEM((SUB, dev * rows, cw), f32), pieces, pieces, pieces, pieces,
            dma((2, SUB)), dma,
        ] + [dma((nm,))] * 4 + [dma((CH, SUB))] * 10,
        compiler_params=pltpu.CompilerParams(collective_id=1, has_side_effects=True, vmem_limit_bytes=48 << 20),
        name="project_out",
    )(*[pltpu.with_memory_space_constraint(a, pltpu.VMEM) for a in (done, last)], Wo, x.reshape(dev, bl, d))
    return y.reshape(b, d)


def _write_kernel(y, k, v, yo, ko, vo, sem):
    copies = [pltpu.make_async_copy(a, b, sem.at[n]) for n, (a, b) in enumerate(((y, yo), (k, ko), (v, vo)))]
    for c in copies:
        c.start()
    for c in copies:
        c.wait()


def _write(y, k, v):
    return pl.pallas_call(
        _write_kernel,
        out_shape=tuple(jax.ShapeDtypeStruct(a.shape, a.dtype) for a in (y, k, v)),
        in_specs=[_vmem()] * 3,
        out_specs=(_hbm(),) * 3,
        scratch_shapes=[pltpu.SemaphoreType.DMA((3,))],
        compiler_params=pltpu.CompilerParams(vmem_limit_bytes=16 << 20),
        name="write",
    )(y, k, v)


def solution(mesh):
    ne = mesh.shape['emb']
    nm = mesh.shape['model']

    def local(x, Wq, Wk, Wv, Wo, Kc, Vc, lengths):
        done, last, k_new, v_new = _attend(x, Wq, Wk, Wv, Kc, Vc, lengths, ne, nm)
        y = _project_out(done, last, Wo, x, ne, nm)
        return _write(y, k_new, v_new)

    in_specs = (P('rep', None), P('emb', 'model'), P(), P(), P('model', 'emb'),
                P('rep', None, None), P('rep', None, None), P('rep'))
    out_specs = (P('rep', None), P('rep', None), P('rep', None))
    return jax.shard_map(local, mesh=mesh, in_specs=in_specs, out_specs=out_specs, check_vma=False)
```

```python
import functools

import jax
import jax.numpy as jnp
from jax import lax
from jax.experimental import pallas as pl
from jax.experimental.pallas import tpu as pltpu
from jax.sharding import PartitionSpec as P

MESH = pl.DeviceIdType.MESH
BK = 512
VLIM = 60
DEAL = 3
RELAY = 2
RING = 6
CH = 8
LAG = 2
SUB = 4
NH = 8


def _vmem():
    return pl.BlockSpec(memory_space=pltpu.VMEM)


def _hbm():
    return pl.BlockSpec(memory_space=pltpu.HBM)


def _smem():
    return pl.BlockSpec(memory_space=pltpu.SMEM)


def _qa_kernel(ne, nm, scale, lens, x, wq, wk, wv, kc, vc, ob, olast, k_out, v_out,
               xv, wqv, wkv, qsend, qrecv, qown, qc, qin, qa, qb, oa, obh, ost, knf, vnf, kbuf, vbuf,
               sa, sb, ma, mb, na, nb_,
               xsem, wsem, kvsem, ss0, sr0, ss, sr, hs, hr, osend, orecv, vsend, vrecv, ksem, vsem):
    i = lax.axis_index("emb")
    j = lax.axis_index("model")
    ie = 1 - i
    de = wq.shape[0]
    be = xv.shape[1] // 2
    bl = be // nm
    rows = bl // CH
    kk = wq.shape[1]
    cw = kk // NH
    dh = wk.shape[1]
    nh = ost.shape[2] // dh
    slots = kc.shape[1]
    start = i * be + j * bl

    def at(a, b):
        return {"emb": a, "model": b}

    def xcopy(a, r):
        row = pl.multiple_of((ie if a == 0 else i) * be, be)
        col = pl.multiple_of((i if r == 0 else ie) * de, de)
        return pltpu.make_async_copy(x.at[pl.ds(row, be), pl.ds(col, de)], xv.at[r, a * be:(a + 1) * be, :], xsem.at[a, r])

    def wcopy(h):
        return pltpu.make_async_copy(wq.at[:, pl.ds(h * cw, cw)], wqv.at[h], wsem.at[h])

    def kvcopy(n, r):
        src = wk if n == 0 else wv
        row = pl.multiple_of((i if r == 0 else ie) * de, de)
        return pltpu.make_async_copy(src.at[pl.ds(row, de), :], wkv.at[n, r], kvsem.at[n, r])

    def kcopy(n):
        slot = lax.rem(n, RING)
        return pltpu.make_async_copy(kc.at[start + n], kbuf.at[slot], ksem.at[slot])

    def vcopy(n):
        slot = lax.rem(n, RING)
        return pltpu.make_async_copy(vc.at[start + n], vbuf.at[slot], vsem.at[slot])

    xcopy(0, 0).start()
    for h in range(NH):
        wcopy(h).start()
    xcopy(1, 0).start()
    xcopy(0, 1).start()
    xcopy(1, 1).start()
    for n in range(2):
        for r in range(2):
            kvcopy(n, r).start()
    for n in range(RING - 1):
        kcopy(n).start()
        if n < RING - 2:
            vcopy(n).start()

    barrier = pltpu.get_barrier_semaphore()
    pl.semaphore_signal(barrier, inc=1, device_id=at(ie, j), device_id_type=MESH)
    for r in range(1, nm):
        pl.semaphore_signal(barrier, inc=1, device_id=at(i, lax.rem(j + r, nm)), device_id_type=MESH)
    pl.semaphore_wait(barrier, nm)

    def first(h):
        return pltpu.make_async_remote_copy(
            src_ref=qsend.at[0, :, pl.ds(h * cw, cw)], dst_ref=qrecv.at[0, :, pl.ds(h * cw, cw)],
            send_sem=ss0.at[h], recv_sem=sr0.at[h], device_id=at(ie, j), device_id_type=MESH)

    def later(s):
        return pltpu.make_async_remote_copy(
            src_ref=qsend.at[s], dst_ref=qrecv.at[s], send_sem=ss.at[s], recv_sem=sr.at[s],
            device_id=at(ie, j), device_id_type=MESH)

    def mycols(d):
        return pl.ds(pl.multiple_of(d * kk, kk), kk)

    def hcopy(s, r):
        d = lax.rem(j + r, nm)
        return pltpu.make_async_remote_copy(
            src_ref=qc.at[s, pl.ds(pl.multiple_of(d * rows, rows), rows), :], dst_ref=qin.at[s, :, mycols(j)],
            send_sem=hs.at[s, r], recv_sem=hr.at[s, nm - r], device_id=at(i, d), device_id_type=MESH)

    def hrecv(s, r):
        d = lax.rem(j + r, nm)
        return pltpu.make_async_remote_copy(
            src_ref=qc.at[s, pl.ds(0, rows), :], dst_ref=qin.at[s, :, mycols(d)],
            send_sem=hs.at[s, r], recv_sem=hr.at[s, r], device_id=at(i, d), device_id_type=MESH)

    def block(a, d):
        return pl.ds(pl.multiple_of((a * nm + d) * rows, rows), rows)

    def ocopy(s, r):
        d = lax.rem(j + r, nm)
        return pltpu.make_async_remote_copy(
            src_ref=ost.at[s, :, mycols(d)], dst_ref=ob.at[s, block(i, j), :],
            send_sem=osend.at[s, r], recv_sem=orecv.at[s, nm - r], device_id=at(i, d), device_id_type=MESH)

    def orecv_copy(s, r):
        d = lax.rem(j + r, nm)
        return pltpu.make_async_remote_copy(
            src_ref=ob.at[s, block(i, d), :], dst_ref=ob.at[s, block(i, d), :],
            send_sem=osend.at[s, r], recv_sem=orecv.at[s, r], device_id=at(i, d), device_id_type=MESH)

    def ycopy(s, r):
        dst = ob.at[s, block(i, lax.rem(j + r, nm)), :]
        return pltpu.make_async_remote_copy(
            src_ref=ost.at[s, :, mycols(j)] if r == 0 else dst, dst_ref=dst,
            send_sem=vsend.at[s, r], recv_sem=vrecv.at[s, r], device_id=at(ie, j), device_id_type=MESH)

    def yrecv_copy(s, r):
        blk = ob.at[s, block(ie, lax.rem(j + r, nm)), :]
        return pltpu.make_async_remote_copy(
            src_ref=blk, dst_ref=blk, send_sem=vsend.at[s, r], recv_sem=vrecv.at[s, r],
            device_id=at(ie, j), device_id_type=MESH)

    def spread(dst, h, val):
        for s in range(CH):
            for d in range(nm):
                dst[s, d * rows:(d + 1) * rows, h * cw:(h + 1) * cw] = val[d * bl + s * rows:d * bl + (s + 1) * rows]

    xcopy(0, 0).wait()
    for h in range(NH):
        wcopy(h).wait()
        spread(qsend, h, jnp.dot(xv[0, :be, :], wqv[h], preferred_element_type=jnp.float32))
        first(h).start()
    for s in range(1, CH):
        later(s).start()
    xcopy(1, 0).wait()
    for h in range(NH):
        spread(qown, h, jnp.dot(xv[0, be:, :], wqv[h], preferred_element_type=jnp.float32))
    def deal(s):
        qc[s] = (qown[s] + qrecv[s]).astype(jnp.bfloat16)
        for r in (2, 3, 1):
            hcopy(s, r).start()
        qin[s, :, mycols(j)] = qc[s, pl.ds(pl.multiple_of(j * rows, rows), rows), :]

    def relay(s):
        for r in range(1, nm):
            orecv_copy(s, r).wait_recv()
            ycopy(s, r).start()

    for h in range(NH):
        first(h).wait_recv()
    deal(0)

    xcopy(0, 1).wait()
    xcopy(1, 1).wait()
    for n in range(2):
        for r in range(2):
            kvcopy(n, r).wait()
    for n, out, rowf in ((0, k_out, knf), (1, v_out, vnf)):
        for a in range(2):
            acc = jnp.dot(xv[0, a * be:(a + 1) * be, :], wkv[n, 0], preferred_element_type=jnp.float32)
            acc += jnp.dot(xv[1, a * be:(a + 1) * be, :], wkv[n, 1], preferred_element_type=jnp.float32)
            out[pl.ds(pl.multiple_of((ie if a == 0 else i) * be, be), be), :] = acc.astype(jnp.bfloat16)
        rowf[...] = out[pl.ds(pl.multiple_of(start, bl), bl), :].astype(jnp.float32)

    def scores(n, sref, mref, nref):
        t = n % rows
        seq = pl.ds(pl.multiple_of(t * nh, nh), nh)
        qf = jnp.concatenate([qa[seq, :], qb[seq, :]], 1)
        q = qf.astype(jnp.bfloat16)
        slot = lax.rem(n, RING)
        new = jnp.sum(qf * knf[pl.ds(n, 1), :], axis=1, keepdims=True) * scale
        count = lens[start + n]
        top = None
        for b in range(slots // BK):
            v = lax.dot_general(q, kbuf[slot, b * BK:(b + 1) * BK, :], (((1,), (1,)), ((), ())),
                                preferred_element_type=jnp.float32) * scale
            v = jnp.where(lax.broadcasted_iota(jnp.int32, v.shape, 1) + b * BK < count, v, -jnp.inf)
            sref[:, b * BK:(b + 1) * BK] = v
            top = v if top is None else jnp.maximum(top, v)
        m = jnp.maximum(jnp.max(top, axis=1, keepdims=True), new)
        mref[...] = jnp.broadcast_to(m, mref.shape)
        nref[...] = jnp.broadcast_to(new, nref.shape)

    def values(n, sref, mref, nref):
        t = n % rows
        seq = pl.ds(pl.multiple_of(t * nh, nh), nh)
        slot = lax.rem(n, RING)
        m = mref[...]
        wide = jnp.concatenate([m] * (BK // 128), 1)
        ps, tot = [], None
        for b in range(slots // BK):
            p = jnp.exp(sref[:, b * BK:(b + 1) * BK] - wide)
            tot = p if tot is None else tot + p
            ps.append(p.astype(jnp.bfloat16))
        acc = jnp.dot(jnp.concatenate(ps, 1), vbuf[slot], preferred_element_type=jnp.float32)
        pn = jnp.exp(nref[...] - m)
        inv = 1.0 / (jnp.sum(tot, axis=1, keepdims=True) + pn)
        pn = pn.astype(jnp.bfloat16).astype(jnp.float32)
        vn = vnf[pl.ds(n, 1), :]
        oa[seq, :] = (acc[:, :128] + pn * vn[:, :128]) * inv
        obh[seq, :] = (acc[:, 128:] + pn * vn[:, 128:]) * inv

    A, B = (sa, ma, na), (sb, mb, nb_)

    def fetch(n):
        @pl.when(n + RING - 1 < bl)
        def _():
            kcopy(n + RING - 1).start()
            vcopy(n + RING - 2).start()

        @pl.when(n + RING - 1 == bl)
        def _():
            vcopy(n + RING - 2).start()

        @pl.when(n + RING < bl)
        def _():
            kcopy(n + RING).start()
            vcopy(n + RING - 1).start()

        @pl.when(n + RING == bl)
        def _():
            vcopy(n + RING - 1).start()

    per = rows // 2

    def load_q(s):
        for r in range(1, nm):
            hrecv(s, r).wait_recv()
        for h in range(nh):
            qa[pl.ds(h, rows, stride=nh), :] = qin[s, :, h * dh:h * dh + 128].astype(jnp.float32)
            qb[pl.ds(h, rows, stride=nh), :] = qin[s, :, h * dh + 128:(h + 1) * dh].astype(jnp.float32)

    def store_o(s):
        for h in range(nh):
            ost[s, :, h * dh:h * dh + 128] = oa[pl.ds(h, rows, stride=nh), :].astype(jnp.bfloat16)
            ost[s, :, h * dh + 128:(h + 1) * dh] = obh[pl.ds(h, rows, stride=nh), :].astype(jnp.bfloat16)

    later(1).wait_recv()
    deal(1)
    load_q(0)
    kcopy(0).wait()
    scores(0, *A)

    def pair(p, c):
        n = 2 * p
        s = p // per
        t = p % per

        @pl.when(t == DEAL)
        def _():
            @pl.when(s + 2 < CH)
            def _():
                later(s + 2).wait_recv()
                deal(s + 2)

        @pl.when(t == RELAY)
        def _():
            @pl.when(s >= 1)
            def _():
                relay(s - 1)

        fetch(n)
        kcopy(n + 1).wait()
        vcopy(n).wait()
        values(n, *A)
        scores(n + 1, *B)

        @pl.when(t == per - 1)
        def _():
            load_q(s + 1)

        kcopy(n + 2).wait()
        vcopy(n + 1).wait()
        values(n + 1, *B)
        scores(n + 2, *A)

        @pl.when(t == per - 1)
        def _():
            store_o(s)
            for r in (2, 3, 1):
                ocopy(s, r).start()
            ycopy(s, 0).start()
            ob[s, block(i, j), :] = ost[s, :, mycols(j)]

        return c

    lax.fori_loop(0, bl // 2 - 1, pair, 0)
    kcopy(bl - 1).wait()
    vcopy(bl - 2).wait()
    values(bl - 2, *A)
    scores(bl - 1, *B)
    vcopy(bl - 1).wait()
    values(bl - 1, *B)
    store_o(CH - 1)
    olast[...] = ost[CH - 1]
    for h in range(NH):
        first(h).wait_send()
    for s in range(CH):
        if s:
            later(s).wait_send()
        for r in range(1, nm):
            hcopy(s, r).wait_send()
            if s < CH - 1:
                ocopy(s, r).wait_send()
        if s < CH - 1:
            for r in range(nm):
                ycopy(s, r).wait_send()
                yrecv_copy(s, r).wait_recv()


def _attend(x, Wq, Wk, Wv, Kc, Vc, lengths, ne, nm):
    b, d = x.shape
    de, kk = Wq.shape
    dh = Wk.shape[1]
    slots = Kc.shape[1]
    be = b // ne
    bl = be // nm
    rows = bl // CH
    cw = kk // NH
    full = kk * nm
    nh = full // dh
    assert dh == 256 and slots % BK == 0
    bf, f32 = jnp.bfloat16, jnp.float32
    dma = pltpu.SemaphoreType.DMA
    V = pltpu.VMEM
    part = V((CH, nm * rows, kk), f32)
    flat = V((rows * nh, 128), f32)
    stat = V((nh, 128), f32)
    return pl.pallas_call(
        functools.partial(_qa_kernel, ne, nm, dh ** -0.5),
        out_shape=(V((CH - 1, b // CH, kk), bf), V((rows, full), bf), V((b, dh), bf), V((b, dh), bf)),
        in_specs=[_smem()] + [_hbm()] * 6,
        out_specs=(_vmem(),) * 4,
        scratch_shapes=[
            V((2, b, de), bf), V((NH, de, cw), bf), V((2, 2, de, dh), bf), part, part, part,
            V((CH, nm * rows, kk), bf), V((CH, rows, full), bf), flat, flat, flat, flat, V((CH, rows, full), bf),
            V((bl, dh), f32), V((bl, dh), f32), V((RING, slots, dh), bf), V((RING, slots, dh), bf),
            V((nh, slots), f32), V((nh, slots), f32), stat, stat, stat, stat,
            dma((2, 2)), dma((NH,)), dma((2, 2)), dma((NH,)), dma((NH,)), dma((CH,)), dma((CH,)),
            dma((CH, nm)), dma((CH, nm)), dma((CH, nm)), dma((CH, nm)), dma((CH, nm)), dma((CH, nm)),
            dma((RING,)), dma((RING,)),
        ],
        compiler_params=pltpu.CompilerParams(collective_id=0, has_side_effects=True, vmem_limit_bytes=VLIM << 20),
        name="attend",
    )(lengths, x, Wq, Wk, Wv, Kc, Vc)


def _out_kernel(ne, nm, od_ref, o_ref, wo, x, y, wv, xv, ob, psend, precv, ssend, srecv,
                wsem, xsem, osend, orecv, vsend, vrecv, ps, pr, xs_, xr, cs, cr, es, er, fs, fr):
    i = lax.axis_index("emb")
    j = lax.axis_index("model")
    c = lax.rem(j, 2)
    jp = j + 1 - 2 * c
    jx = lax.rem(j + 2, nm)
    ie = 1 - i
    half = wv.shape[2]
    cw = half // SUB
    rows = o_ref.shape[0]
    kk = wv.shape[1]
    dev = ne * nm

    def at(a, b):
        return {"emb": a, "model": b}

    def wcopy(b, u):
        col = pl.multiple_of((1 - c if b == 0 else c) * half + u * cw, cw)
        return pltpu.make_async_copy(wo.at[:, pl.ds(col, cw)], wv.at[b, :, pl.ds(u * cw, cw)], wsem.at[b, u])

    order = [(0, 0)] + [p for u in range(1, SUB) for p in ((0, u), (1, u - 1))] + [(1, SUB - 1)]
    for b, u in order:
        wcopy(b, u).start()
    mycol = pl.multiple_of((i * 2 + c) * half, half)
    excol = pl.multiple_of((ie * 2 + c) * half, half)
    xcopy = pltpu.make_async_copy(x.at[:, :, pl.ds(mycol, half)], xv, xsem)
    xcopy.start()

    barrier = pltpu.get_barrier_semaphore()
    pl.semaphore_signal(barrier, inc=1, device_id=at(ie, j), device_id_type=MESH)
    for r in range(1, nm):
        pl.semaphore_signal(barrier, inc=1, device_id=at(i, lax.rem(j + r, nm)), device_id_type=MESH)
    pl.semaphore_wait(barrier, nm)

    def block(a, d):
        return pl.ds(pl.multiple_of((a * nm + d) * rows, rows), rows)

    def heads(d):
        return pl.ds(pl.multiple_of(d * kk, kk), kk)

    def ocopy(r):
        d = lax.rem(j + r, nm)
        return pltpu.make_async_remote_copy(
            src_ref=o_ref.at[:, heads(d)], dst_ref=ob.at[block(i, j), :],
            send_sem=osend.at[r], recv_sem=orecv.at[nm - r], device_id=at(i, d), device_id_type=MESH)

    def orecv_copy(r):
        d = lax.rem(j + r, nm)
        return pltpu.make_async_remote_copy(
            src_ref=ob.at[block(i, d), :], dst_ref=ob.at[block(i, d), :],
            send_sem=osend.at[r], recv_sem=orecv.at[r], device_id=at(i, d), device_id_type=MESH)

    def vcopy(r):
        dst = ob.at[block(i, lax.rem(j + r, nm)), :]
        return pltpu.make_async_remote_copy(
            src_ref=o_ref.at[:, heads(j)] if r == 0 else dst, dst_ref=dst,
            send_sem=vsend.at[r], recv_sem=vrecv.at[r], device_id=at(ie, j), device_id_type=MESH)

    def vrecv_copy(r):
        blk = ob.at[block(ie, lax.rem(j + r, nm)), :]
        return pltpu.make_async_remote_copy(
            src_ref=blk, dst_ref=blk, send_sem=vsend.at[r], recv_sem=vrecv.at[r],
            device_id=at(ie, j), device_id_type=MESH)

    for r in (2, 3, 1):
        ocopy(r).start()
    vcopy(0).start()
    ob[block(i, j), :] = o_ref[:, heads(j)]

    def pcopy(s, u):
        return pltpu.make_async_remote_copy(
            src_ref=psend.at[s, u], dst_ref=precv.at[s, u], send_sem=ps.at[s, u], recv_sem=pr.at[s, u],
            device_id=at(i, jp), device_id_type=MESH)

    def scopy(s, u):
        return pltpu.make_async_remote_copy(
            src_ref=ssend.at[s, u], dst_ref=srecv.at[s, u], send_sem=xs_.at[s, u], recv_sem=xr.at[s, u],
            device_id=at(i, jx), device_id_type=MESH)

    def piece(s, u, base):
        return y.at[:, pl.ds(pl.multiple_of(s * rows, rows), rows), pl.ds(pl.multiple_of(base + u * cw, cw), cw)]

    def ccopy(s, u):
        return pltpu.make_async_remote_copy(
            src_ref=piece(s, u, mycol), dst_ref=piece(s, u, mycol), send_sem=cs.at[s, u], recv_sem=cr.at[s, u],
            device_id=at(i, jp), device_id_type=MESH)

    def ecopy(s, u):
        return pltpu.make_async_remote_copy(
            src_ref=piece(s, u, mycol), dst_ref=piece(s, u, mycol), send_sem=es.at[s, u], recv_sem=er.at[s, u],
            device_id=at(ie, j), device_id_type=MESH)

    def fcopy(s, u):
        return pltpu.make_async_remote_copy(
            src_ref=piece(s, u, excol), dst_ref=piece(s, u, excol), send_sem=fs.at[s, u], recv_sem=fr.at[s, u],
            device_id=at(i, jp), device_id_type=MESH)

    def compute(s, lhs):
        for b, u in order:
            @pl.when(s == 0)
            def _():
                wcopy(b, u).wait()

            part = jnp.dot(lhs(), wv[b, :, u * cw:(u + 1) * cw], preferred_element_type=jnp.float32)
            if b == 0:
                psend[s, u] = part.astype(jnp.bfloat16)
                pcopy(s, u).start()
            else:
                pcopy(s, u).wait_recv()
                ssend[s, u] = (part + precv[s, u].astype(jnp.float32)).astype(jnp.bfloat16)
                scopy(s, u).start()

    def finish(s):
        at_rows = pl.ds(pl.multiple_of(s * rows, rows), rows)
        for u in range(SUB):
            scopy(s, u).wait_recv()
            tot = ssend[s, u].astype(jnp.float32) + srecv[s, u].astype(jnp.float32)
            xs = xv[:, at_rows, u * cw:(u + 1) * cw].astype(jnp.float32)
            y[:, at_rows, pl.ds(pl.multiple_of(mycol + u * cw, cw), cw)] = (
                xs + tot.reshape(dev, rows, cw)).astype(jnp.bfloat16)
            ecopy(s, u).start()
            ccopy(s, u).start()

    def forward(s):
        for u in range(SUB):
            ecopy(s, u).wait_recv()
            fcopy(s, u).start()

    def step(s, carry):
        compute(s, lambda: od_ref[s])

        @pl.when(s == 0)
        def _():
            for r in range(1, nm):
                orecv_copy(r).wait_recv()
                vcopy(r).start()
            xcopy.wait()

        @pl.when(s >= LAG)
        def _():
            finish(s - LAG)

        @pl.when(s >= 2 * LAG)
        def _():
            forward(s - 2 * LAG)

        return carry

    lax.fori_loop(0, CH - 1, step, 0)
    for r in range(nm):
        vrecv_copy(r).wait_recv()
    compute(CH - 1, lambda: ob[...])
    for s in range(CH - 1, CH + LAG):
        finish(s - LAG)
        forward(s - 2 * LAG)
    for s in range(CH - LAG, CH):
        forward(s)
    for r in range(1, nm):
        ocopy(r).wait_send()
    for r in range(nm):
        vcopy(r).wait_send()
    for s in range(CH):
        for u in range(SUB):
            pcopy(s, u).wait_send()
            scopy(s, u).wait_send()
            ecopy(s, u).wait_send()
            ccopy(s, u).wait()
            fcopy(s, u).wait()


def _project_out(done, last, Wo, x, ne, nm):
    bl = CH * last.shape[0]
    kk, ncol = Wo.shape
    half = ncol // 2
    dev = ne * nm
    rows = bl // CH
    cw = half // SUB
    b, d = x.shape
    bf, f32 = jnp.bfloat16, jnp.float32
    dma = pltpu.SemaphoreType.DMA
    pieces = pltpu.VMEM((CH, SUB, dev * rows, cw), bf)
    y = pl.pallas_call(
        functools.partial(_out_kernel, ne, nm),
        out_shape=pltpu.VMEM((dev, bl, d), bf),
        in_specs=[_vmem(), _vmem(), _hbm(), _hbm()],
        out_specs=_vmem(),
        scratch_shapes=[
            pltpu.VMEM((2, kk, half), bf), pltpu.VMEM((dev, bl, half), bf), pltpu.VMEM((dev * rows, kk), bf),
            pieces, pieces, pieces, pieces,
            dma((2, SUB)), dma,
        ] + [dma((nm,))] * 4 + [dma((CH, SUB))] * 10,
        compiler_params=pltpu.CompilerParams(collective_id=1, has_side_effects=True, vmem_limit_bytes=48 << 20),
        name="project_out",
    )(*[pltpu.with_memory_space_constraint(a, pltpu.VMEM) for a in (done, last)], Wo, x.reshape(dev, bl, d))
    return y.reshape(b, d)


def _write_kernel(y, k, v, yo, ko, vo, sem):
    copies = [pltpu.make_async_copy(a, b, sem.at[n]) for n, (a, b) in enumerate(((y, yo), (k, ko), (v, vo)))]
    for c in copies:
        c.start()
    for c in copies:
        c.wait()


def _write(y, k, v):
    return pl.pallas_call(
        _write_kernel,
        out_shape=tuple(jax.ShapeDtypeStruct(a.shape, a.dtype) for a in (y, k, v)),
        in_specs=[_vmem()] * 3,
        out_specs=(_hbm(),) * 3,
        scratch_shapes=[pltpu.SemaphoreType.DMA((3,))],
        compiler_params=pltpu.CompilerParams(vmem_limit_bytes=16 << 20),
        name="write",
    )(y, k, v)


def solution(mesh):
    ne = mesh.shape['emb']
    nm = mesh.shape['model']

    def local(x, Wq, Wk, Wv, Wo, Kc, Vc, lengths):
        done, last, k_new, v_new = _attend(x, Wq, Wk, Wv, Kc, Vc, lengths, ne, nm)
        y = _project_out(done, last, Wo, x, ne, nm)
        return _write(y, k_new, v_new)

    in_specs = (P('rep', None), P('emb', 'model'), P(), P(), P('model', 'emb'),
                P('rep', None, None), P('rep', None, None), P('rep'))
    out_specs = (P('rep', None), P('rep', None), P('rep', None))
    return jax.shard_map(local, mesh=mesh, in_specs=in_specs, out_specs=out_specs, check_vma=False)
```

```python
import functools

import jax
import jax.numpy as jnp
from jax import lax
from jax.experimental import pallas as pl
from jax.experimental.pallas import tpu as pltpu
from jax.sharding import PartitionSpec as P

MESH = pl.DeviceIdType.MESH
BK = 512
VLIM = 60
DEAL = 3
CUT = 4
RELAY = 2
RING = 6
CH = 8
LAG = 2
SUB = 4
NH = 8


def _vmem():
    return pl.BlockSpec(memory_space=pltpu.VMEM)


def _hbm():
    return pl.BlockSpec(memory_space=pltpu.HBM)


def _smem():
    return pl.BlockSpec(memory_space=pltpu.SMEM)


def _qa_kernel(ne, nm, scale, lens, x, wq, wk, wv, kc, vc, ob, olast, k_out, v_out,
               xv, wqv, wkv, qsend, qrecv, qown, qc, qin, qa, qb, oa, obh, ost, knf, vnf, kbuf, vbuf,
               sa, sb, ma, mb, na, nb_,
               xsem, wsem, kvsem, ss0, sr0, ss, sr, hs, hr, osend, orecv, vsend, vrecv, ksem, vsem):
    i = lax.axis_index("emb")
    j = lax.axis_index("model")
    ie = 1 - i
    de = wq.shape[0]
    be = xv.shape[1] // 2
    bl = be // nm
    rows = bl // CH
    kk = wq.shape[1]
    cw = kk // NH
    dh = wk.shape[1]
    nh = ost.shape[2] // dh
    slots = kc.shape[1]
    start = i * be + j * bl

    def at(a, b):
        return {"emb": a, "model": b}

    def xcopy(a, r):
        row = pl.multiple_of((ie if a == 0 else i) * be, be)
        col = pl.multiple_of((i if r == 0 else ie) * de, de)
        return pltpu.make_async_copy(x.at[pl.ds(row, be), pl.ds(col, de)], xv.at[r, a * be:(a + 1) * be, :], xsem.at[a, r])

    def wcopy(h):
        return pltpu.make_async_copy(wq.at[:, pl.ds(h * cw, cw)], wqv.at[h], wsem.at[h])

    def kvcopy(n, r):
        src = wk if n == 0 else wv
        row = pl.multiple_of((i if r == 0 else ie) * de, de)
        return pltpu.make_async_copy(src.at[pl.ds(row, de), :], wkv.at[n, r], kvsem.at[n, r])

    class Pieces:
        def __init__(self, src, dst, sem, n):
            slot, w = lax.rem(n, RING), slots // CUT
            self.copies = [pltpu.make_async_copy(src.at[start + n, pl.ds(k * w, w)], dst.at[slot, pl.ds(k * w, w)],
                                                 sem.at[slot, k]) for k in range(CUT)]

        def start(self):
            for a in self.copies:
                a.start()

        def wait(self):
            for a in self.copies:
                a.wait()

    def kcopy(n):
        return Pieces(kc, kbuf, ksem, n)

    def vcopy(n):
        return Pieces(vc, vbuf, vsem, n)

    xcopy(0, 0).start()
    for h in range(NH):
        wcopy(h).start()
    xcopy(1, 0).start()
    xcopy(0, 1).start()
    xcopy(1, 1).start()
    for n in range(2):
        for r in range(2):
            kvcopy(n, r).start()
    for n in range(RING - 1):
        kcopy(n).start()
        if n < RING - 2:
            vcopy(n).start()

    barrier = pltpu.get_barrier_semaphore()
    pl.semaphore_signal(barrier, inc=1, device_id=at(ie, j), device_id_type=MESH)
    for r in range(1, nm):
        pl.semaphore_signal(barrier, inc=1, device_id=at(i, lax.rem(j + r, nm)), device_id_type=MESH)
    pl.semaphore_wait(barrier, nm)

    def first(h):
        return pltpu.make_async_remote_copy(
            src_ref=qsend.at[0, :, pl.ds(h * cw, cw)], dst_ref=qrecv.at[0, :, pl.ds(h * cw, cw)],
            send_sem=ss0.at[h], recv_sem=sr0.at[h], device_id=at(ie, j), device_id_type=MESH)

    def later(s):
        return pltpu.make_async_remote_copy(
            src_ref=qsend.at[s], dst_ref=qrecv.at[s], send_sem=ss.at[s], recv_sem=sr.at[s],
            device_id=at(ie, j), device_id_type=MESH)

    def mycols(d):
        return pl.ds(pl.multiple_of(d * kk, kk), kk)

    def hcopy(s, r):
        d = lax.rem(j + r, nm)
        return pltpu.make_async_remote_copy(
            src_ref=qc.at[s, pl.ds(pl.multiple_of(d * rows, rows), rows), :], dst_ref=qin.at[s, :, mycols(j)],
            send_sem=hs.at[s, r], recv_sem=hr.at[s, nm - r], device_id=at(i, d), device_id_type=MESH)

    def hrecv(s, r):
        d = lax.rem(j + r, nm)
        return pltpu.make_async_remote_copy(
            src_ref=qc.at[s, pl.ds(0, rows), :], dst_ref=qin.at[s, :, mycols(d)],
            send_sem=hs.at[s, r], recv_sem=hr.at[s, r], device_id=at(i, d), device_id_type=MESH)

    def block(a, d):
        return pl.ds(pl.multiple_of((a * nm + d) * rows, rows), rows)

    def ocopy(s, r):
        d = lax.rem(j + r, nm)
        return pltpu.make_async_remote_copy(
            src_ref=ost.at[s, :, mycols(d)], dst_ref=ob.at[s, block(i, j), :],
            send_sem=osend.at[s, r], recv_sem=orecv.at[s, nm - r], device_id=at(i, d), device_id_type=MESH)

    def orecv_copy(s, r):
        d = lax.rem(j + r, nm)
        return pltpu.make_async_remote_copy(
            src_ref=ob.at[s, block(i, d), :], dst_ref=ob.at[s, block(i, d), :],
            send_sem=osend.at[s, r], recv_sem=orecv.at[s, r], device_id=at(i, d), device_id_type=MESH)

    def ycopy(s, r):
        dst = ob.at[s, block(i, lax.rem(j + r, nm)), :]
        return pltpu.make_async_remote_copy(
            src_ref=ost.at[s, :, mycols(j)] if r == 0 else dst, dst_ref=dst,
            send_sem=vsend.at[s, r], recv_sem=vrecv.at[s, r], device_id=at(ie, j), device_id_type=MESH)

    def yrecv_copy(s, r):
        blk = ob.at[s, block(ie, lax.rem(j + r, nm)), :]
        return pltpu.make_async_remote_copy(
            src_ref=blk, dst_ref=blk, send_sem=vsend.at[s, r], recv_sem=vrecv.at[s, r],
            device_id=at(ie, j), device_id_type=MESH)

    def spread(dst, h, val):
        for s in range(CH):
            for d in range(nm):
                dst[s, d * rows:(d + 1) * rows, h * cw:(h + 1) * cw] = val[d * bl + s * rows:d * bl + (s + 1) * rows]

    xcopy(0, 0).wait()
    for h in range(NH):
        wcopy(h).wait()
        spread(qsend, h, jnp.dot(xv[0, :be, :], wqv[h], preferred_element_type=jnp.float32))
        first(h).start()
    for s in range(1, CH):
        later(s).start()
    xcopy(1, 0).wait()
    for h in range(NH):
        spread(qown, h, jnp.dot(xv[0, be:, :], wqv[h], preferred_element_type=jnp.float32))
    def deal(s):
        qc[s] = (qown[s] + qrecv[s]).astype(jnp.bfloat16)
        for r in (2, 3, 1):
            hcopy(s, r).start()
        qin[s, :, mycols(j)] = qc[s, pl.ds(pl.multiple_of(j * rows, rows), rows), :]

    def relay(s):
        for r in range(1, nm):
            orecv_copy(s, r).wait_recv()
            ycopy(s, r).start()

    for h in range(NH):
        first(h).wait_recv()
    deal(0)

    xcopy(0, 1).wait()
    xcopy(1, 1).wait()
    for n in range(2):
        for r in range(2):
            kvcopy(n, r).wait()
    for n, out, rowf in ((0, k_out, knf), (1, v_out, vnf)):
        for a in range(2):
            acc = jnp.dot(xv[0, a * be:(a + 1) * be, :], wkv[n, 0], preferred_element_type=jnp.float32)
            acc += jnp.dot(xv[1, a * be:(a + 1) * be, :], wkv[n, 1], preferred_element_type=jnp.float32)
            out[pl.ds(pl.multiple_of((ie if a == 0 else i) * be, be), be), :] = acc.astype(jnp.bfloat16)
        rowf[...] = out[pl.ds(pl.multiple_of(start, bl), bl), :].astype(jnp.float32)

    def scores(n, sref, mref, nref):
        t = n % rows
        seq = pl.ds(pl.multiple_of(t * nh, nh), nh)
        qf = jnp.concatenate([qa[seq, :], qb[seq, :]], 1)
        q = qf.astype(jnp.bfloat16)
        slot = lax.rem(n, RING)
        new = jnp.sum(qf * knf[pl.ds(n, 1), :], axis=1, keepdims=True) * scale
        count = lens[start + n]
        top = None
        for b in range(slots // BK):
            v = lax.dot_general(q, kbuf[slot, b * BK:(b + 1) * BK, :], (((1,), (1,)), ((), ())),
                                preferred_element_type=jnp.float32) * scale
            v = jnp.where(lax.broadcasted_iota(jnp.int32, v.shape, 1) + b * BK < count, v, -jnp.inf)
            sref[:, b * BK:(b + 1) * BK] = v
            top = v if top is None else jnp.maximum(top, v)
        m = jnp.maximum(jnp.max(top, axis=1, keepdims=True), new)
        mref[...] = jnp.broadcast_to(m, mref.shape)
        nref[...] = jnp.broadcast_to(new, nref.shape)

    def values(n, sref, mref, nref):
        t = n % rows
        seq = pl.ds(pl.multiple_of(t * nh, nh), nh)
        slot = lax.rem(n, RING)
        m = mref[...]
        wide = jnp.concatenate([m] * (BK // 128), 1)
        ps, tot = [], None
        for b in range(slots // BK):
            p = jnp.exp(sref[:, b * BK:(b + 1) * BK] - wide)
            tot = p if tot is None else tot + p
            ps.append(p.astype(jnp.bfloat16))
        acc = jnp.dot(jnp.concatenate(ps, 1), vbuf[slot], preferred_element_type=jnp.float32)
        pn = jnp.exp(nref[...] - m)
        inv = 1.0 / (jnp.sum(tot, axis=1, keepdims=True) + pn)
        pn = pn.astype(jnp.bfloat16).astype(jnp.float32)
        vn = vnf[pl.ds(n, 1), :]
        oa[seq, :] = (acc[:, :128] + pn * vn[:, :128]) * inv
        obh[seq, :] = (acc[:, 128:] + pn * vn[:, 128:]) * inv

    A, B = (sa, ma, na), (sb, mb, nb_)

    def fetch(n):
        @pl.when(n + RING - 1 < bl)
        def _():
            kcopy(n + RING - 1).start()
            vcopy(n + RING - 2).start()

        @pl.when(n + RING - 1 == bl)
        def _():
            vcopy(n + RING - 2).start()

        @pl.when(n + RING < bl)
        def _():
            kcopy(n + RING).start()
            vcopy(n + RING - 1).start()

        @pl.when(n + RING == bl)
        def _():
            vcopy(n + RING - 1).start()

    per = rows // 2

    def load_q(s):
        for r in range(1, nm):
            hrecv(s, r).wait_recv()
        for h in range(nh):
            qa[pl.ds(h, rows, stride=nh), :] = qin[s, :, h * dh:h * dh + 128].astype(jnp.float32)
            qb[pl.ds(h, rows, stride=nh), :] = qin[s, :, h * dh + 128:(h + 1) * dh].astype(jnp.float32)

    def store_o(s):
        for h in range(nh):
            ost[s, :, h * dh:h * dh + 128] = oa[pl.ds(h, rows, stride=nh), :].astype(jnp.bfloat16)
            ost[s, :, h * dh + 128:(h + 1) * dh] = obh[pl.ds(h, rows, stride=nh), :].astype(jnp.bfloat16)

    later(1).wait_recv()
    deal(1)
    load_q(0)
    kcopy(0).wait()
    scores(0, *A)

    def pair(p, c):
        n = 2 * p
        s = p // per
        t = p % per

        @pl.when(t == DEAL)
        def _():
            @pl.when(s + 2 < CH)
            def _():
                later(s + 2).wait_recv()
                deal(s + 2)

        @pl.when(t == RELAY)
        def _():
            @pl.when(s >= 1)
            def _():
                relay(s - 1)

        fetch(n)
        kcopy(n + 1).wait()
        vcopy(n).wait()
        values(n, *A)
        scores(n + 1, *B)

        @pl.when(t == per - 1)
        def _():
            load_q(s + 1)

        kcopy(n + 2).wait()
        vcopy(n + 1).wait()
        values(n + 1, *B)
        scores(n + 2, *A)

        @pl.when(t == per - 1)
        def _():
            store_o(s)
            for r in (2, 3, 1):
                ocopy(s, r).start()
            ycopy(s, 0).start()
            ob[s, block(i, j), :] = ost[s, :, mycols(j)]

        return c

    lax.fori_loop(0, bl // 2 - 1, pair, 0)
    kcopy(bl - 1).wait()
    vcopy(bl - 2).wait()
    values(bl - 2, *A)
    scores(bl - 1, *B)
    vcopy(bl - 1).wait()
    values(bl - 1, *B)
    store_o(CH - 1)
    olast[...] = ost[CH - 1]
    for h in range(NH):
        first(h).wait_send()
    for s in range(CH):
        if s:
            later(s).wait_send()
        for r in range(1, nm):
            hcopy(s, r).wait_send()
            if s < CH - 1:
                ocopy(s, r).wait_send()
        if s < CH - 1:
            for r in range(nm):
                ycopy(s, r).wait_send()
                yrecv_copy(s, r).wait_recv()


def _attend(x, Wq, Wk, Wv, Kc, Vc, lengths, ne, nm):
    b, d = x.shape
    de, kk = Wq.shape
    dh = Wk.shape[1]
    slots = Kc.shape[1]
    be = b // ne
    bl = be // nm
    rows = bl // CH
    cw = kk // NH
    full = kk * nm
    nh = full // dh
    assert dh == 256 and slots % BK == 0
    bf, f32 = jnp.bfloat16, jnp.float32
    dma = pltpu.SemaphoreType.DMA
    V = pltpu.VMEM
    part = V((CH, nm * rows, kk), f32)
    flat = V((rows * nh, 128), f32)
    stat = V((nh, 128), f32)
    return pl.pallas_call(
        functools.partial(_qa_kernel, ne, nm, dh ** -0.5),
        out_shape=(V((CH - 1, b // CH, kk), bf), V((rows, full), bf), V((b, dh), bf), V((b, dh), bf)),
        in_specs=[_smem()] + [_hbm()] * 6,
        out_specs=(_vmem(),) * 4,
        scratch_shapes=[
            V((2, b, de), bf), V((NH, de, cw), bf), V((2, 2, de, dh), bf), part, part, part,
            V((CH, nm * rows, kk), bf), V((CH, rows, full), bf), flat, flat, flat, flat, V((CH, rows, full), bf),
            V((bl, dh), f32), V((bl, dh), f32), V((RING, slots, dh), bf), V((RING, slots, dh), bf),
            V((nh, slots), f32), V((nh, slots), f32), stat, stat, stat, stat,
            dma((2, 2)), dma((NH,)), dma((2, 2)), dma((NH,)), dma((NH,)), dma((CH,)), dma((CH,)),
            dma((CH, nm)), dma((CH, nm)), dma((CH, nm)), dma((CH, nm)), dma((CH, nm)), dma((CH, nm)),
            dma((RING, CUT)), dma((RING, CUT)),
        ],
        compiler_params=pltpu.CompilerParams(collective_id=0, has_side_effects=True, vmem_limit_bytes=VLIM << 20),
        name="attend",
    )(lengths, x, Wq, Wk, Wv, Kc, Vc)


def _out_kernel(ne, nm, od_ref, o_ref, wo, x, y, wv, xv, ob, pown, psend, precv, ssend, srecv,
                wsem, xsem, osend, orecv, vsend, vrecv, ps, pr, xs_, xr, cs, cr, es, er, fs, fr):
    i = lax.axis_index("emb")
    j = lax.axis_index("model")
    c = lax.rem(j, 2)
    jp = j + 1 - 2 * c
    jx = lax.rem(j + 2, nm)
    ie = 1 - i
    half = wv.shape[2]
    cw = half // SUB
    rows = o_ref.shape[0]
    kk = wv.shape[1]
    dev = ne * nm

    def at(a, b):
        return {"emb": a, "model": b}

    def wcopy(b, u):
        col = pl.multiple_of((1 - c if b == 0 else c) * half + u * cw, cw)
        return pltpu.make_async_copy(wo.at[:, pl.ds(col, cw)], wv.at[b, :, pl.ds(u * cw, cw)], wsem.at[b, u])

    for b in range(2):
        for u in range(SUB):
            wcopy(b, u).start()
    mycol = pl.multiple_of((i * 2 + c) * half, half)
    excol = pl.multiple_of((ie * 2 + c) * half, half)
    xcopy = pltpu.make_async_copy(x.at[:, :, pl.ds(mycol, half)], xv, xsem)
    xcopy.start()

    barrier = pltpu.get_barrier_semaphore()
    pl.semaphore_signal(barrier, inc=1, device_id=at(ie, j), device_id_type=MESH)
    for r in range(1, nm):
        pl.semaphore_signal(barrier, inc=1, device_id=at(i, lax.rem(j + r, nm)), device_id_type=MESH)
    pl.semaphore_wait(barrier, nm)

    def block(a, d):
        return pl.ds(pl.multiple_of((a * nm + d) * rows, rows), rows)

    def heads(d):
        return pl.ds(pl.multiple_of(d * kk, kk), kk)

    def ocopy(r):
        d = lax.rem(j + r, nm)
        return pltpu.make_async_remote_copy(
            src_ref=o_ref.at[:, heads(d)], dst_ref=ob.at[block(i, j), :],
            send_sem=osend.at[r], recv_sem=orecv.at[nm - r], device_id=at(i, d), device_id_type=MESH)

    def orecv_copy(r):
        d = lax.rem(j + r, nm)
        return pltpu.make_async_remote_copy(
            src_ref=ob.at[block(i, d), :], dst_ref=ob.at[block(i, d), :],
            send_sem=osend.at[r], recv_sem=orecv.at[r], device_id=at(i, d), device_id_type=MESH)

    def vcopy(r):
        dst = ob.at[block(i, lax.rem(j + r, nm)), :]
        return pltpu.make_async_remote_copy(
            src_ref=o_ref.at[:, heads(j)] if r == 0 else dst, dst_ref=dst,
            send_sem=vsend.at[r], recv_sem=vrecv.at[r], device_id=at(ie, j), device_id_type=MESH)

    def vrecv_copy(r):
        blk = ob.at[block(ie, lax.rem(j + r, nm)), :]
        return pltpu.make_async_remote_copy(
            src_ref=blk, dst_ref=blk, send_sem=vsend.at[r], recv_sem=vrecv.at[r],
            device_id=at(ie, j), device_id_type=MESH)

    for r in (2, 3, 1):
        ocopy(r).start()
    vcopy(0).start()
    ob[block(i, j), :] = o_ref[:, heads(j)]

    def pcopy(s, u):
        return pltpu.make_async_remote_copy(
            src_ref=psend.at[s, u], dst_ref=precv.at[s, u], send_sem=ps.at[s, u], recv_sem=pr.at[s, u],
            device_id=at(i, jp), device_id_type=MESH)

    def scopy(s, u):
        return pltpu.make_async_remote_copy(
            src_ref=ssend.at[s, u], dst_ref=srecv.at[s, u], send_sem=xs_.at[s, u], recv_sem=xr.at[s, u],
            device_id=at(i, jx), device_id_type=MESH)

    def piece(s, u, base):
        return y.at[:, pl.ds(pl.multiple_of(s * rows, rows), rows), pl.ds(pl.multiple_of(base + u * cw, cw), cw)]

    def ccopy(s, u):
        return pltpu.make_async_remote_copy(
            src_ref=piece(s, u, mycol), dst_ref=piece(s, u, mycol), send_sem=cs.at[s, u], recv_sem=cr.at[s, u],
            device_id=at(i, jp), device_id_type=MESH)

    def ecopy(s, u):
        return pltpu.make_async_remote_copy(
            src_ref=piece(s, u, mycol), dst_ref=piece(s, u, mycol), send_sem=es.at[s, u], recv_sem=er.at[s, u],
            device_id=at(ie, j), device_id_type=MESH)

    def fcopy(s, u):
        return pltpu.make_async_remote_copy(
            src_ref=piece(s, u, excol), dst_ref=piece(s, u, excol), send_sem=fs.at[s, u], recv_sem=fr.at[s, u],
            device_id=at(i, jp), device_id_type=MESH)

    def compute(s, lhs):
        for u in range(SUB):
            @pl.when(s == 0)
            def _():
                wcopy(0, u).wait()

            psend[s, u] = jnp.dot(lhs(), wv[0, :, u * cw:(u + 1) * cw],
                                  preferred_element_type=jnp.float32).astype(jnp.bfloat16)
            pcopy(s, u).start()
        for u in range(SUB):
            @pl.when(s == 0)
            def _():
                wcopy(1, u).wait()

            pown[u] = jnp.dot(lhs(), wv[1, :, u * cw:(u + 1) * cw], preferred_element_type=jnp.float32)
            pcopy(s, u).wait_recv()
            ssend[s, u] = (pown[u] + precv[s, u].astype(jnp.float32)).astype(jnp.bfloat16)
            scopy(s, u).start()

    def finish(s):
        at_rows = pl.ds(pl.multiple_of(s * rows, rows), rows)
        for u in range(SUB):
            scopy(s, u).wait_recv()
            tot = ssend[s, u].astype(jnp.float32) + srecv[s, u].astype(jnp.float32)
            xs = xv[:, at_rows, u * cw:(u + 1) * cw].astype(jnp.float32)
            y[:, at_rows, pl.ds(pl.multiple_of(mycol + u * cw, cw), cw)] = (
                xs + tot.reshape(dev, rows, cw)).astype(jnp.bfloat16)
            ecopy(s, u).start()
            ccopy(s, u).start()

    def forward(s):
        for u in range(SUB):
            ecopy(s, u).wait_recv()
            fcopy(s, u).start()

    def step(s, carry):
        compute(s, lambda: od_ref[s])

        @pl.when(s == 0)
        def _():
            for r in range(1, nm):
                orecv_copy(r).wait_recv()
                vcopy(r).start()
            xcopy.wait()

        @pl.when(s >= LAG)
        def _():
            finish(s - LAG)

        @pl.when(s >= 2 * LAG)
        def _():
            forward(s - 2 * LAG)

        return carry

    lax.fori_loop(0, CH - 1, step, 0)
    for r in range(nm):
        vrecv_copy(r).wait_recv()
    compute(CH - 1, lambda: ob[...])
    for s in range(CH - 1, CH + LAG):
        finish(s - LAG)
        forward(s - 2 * LAG)
    for s in range(CH - LAG, CH):
        forward(s)
    for r in range(1, nm):
        ocopy(r).wait_send()
    for r in range(nm):
        vcopy(r).wait_send()
    for s in range(CH):
        for u in range(SUB):
            pcopy(s, u).wait_send()
            scopy(s, u).wait_send()
            ecopy(s, u).wait_send()
            ccopy(s, u).wait()
            fcopy(s, u).wait()


def _project_out(done, last, Wo, x, ne, nm):
    bl = CH * last.shape[0]
    kk, ncol = Wo.shape
    half = ncol // 2
    dev = ne * nm
    rows = bl // CH
    cw = half // SUB
    b, d = x.shape
    bf, f32 = jnp.bfloat16, jnp.float32
    dma = pltpu.SemaphoreType.DMA
    pieces = pltpu.VMEM((CH, SUB, dev * rows, cw), bf)
    y = pl.pallas_call(
        functools.partial(_out_kernel, ne, nm),
        out_shape=pltpu.VMEM((dev, bl, d), bf),
        in_specs=[_vmem(), _vmem(), _hbm(), _hbm()],
        out_specs=_vmem(),
        scratch_shapes=[
            pltpu.VMEM((2, kk, half), bf), pltpu.VMEM((dev, bl, half), bf), pltpu.VMEM((dev * rows, kk), bf),
            pltpu.VMEM((SUB, dev * rows, cw), f32), pieces, pieces, pieces, pieces,
            dma((2, SUB)), dma,
        ] + [dma((nm,))] * 4 + [dma((CH, SUB))] * 10,
        compiler_params=pltpu.CompilerParams(collective_id=1, has_side_effects=True, vmem_limit_bytes=48 << 20),
        name="project_out",
    )(*[pltpu.with_memory_space_constraint(a, pltpu.VMEM) for a in (done, last)], Wo, x.reshape(dev, bl, d))
    return y.reshape(b, d)


def _write_kernel(y, k, v, yo, ko, vo, sem):
    copies = [pltpu.make_async_copy(a, b, sem.at[n]) for n, (a, b) in enumerate(((y, yo), (k, ko), (v, vo)))]
    for c in copies:
        c.start()
    for c in copies:
        c.wait()


def _write(y, k, v):
    return pl.pallas_call(
        _write_kernel,
        out_shape=tuple(jax.ShapeDtypeStruct(a.shape, a.dtype) for a in (y, k, v)),
        in_specs=[_vmem()] * 3,
        out_specs=(_hbm(),) * 3,
        scratch_shapes=[pltpu.SemaphoreType.DMA((3,))],
        compiler_params=pltpu.CompilerParams(vmem_limit_bytes=16 << 20),
        name="write",
    )(y, k, v)


def solution(mesh):
    ne = mesh.shape['emb']
    nm = mesh.shape['model']

    def local(x, Wq, Wk, Wv, Wo, Kc, Vc, lengths):
        done, last, k_new, v_new = _attend(x, Wq, Wk, Wv, Kc, Vc, lengths, ne, nm)
        y = _project_out(done, last, Wo, x, ne, nm)
        return _write(y, k_new, v_new)

    in_specs = (P('rep', None), P('emb', 'model'), P(), P(), P('model', 'emb'),
                P('rep', None, None), P('rep', None, None), P('rep'))
    out_specs = (P('rep', None), P('rep', None), P('rep', None))
    return jax.shard_map(local, mesh=mesh, in_specs=in_specs, out_specs=out_specs, check_vma=False)
```

```python
import functools

import jax
import jax.numpy as jnp
from jax import lax
from jax.experimental import pallas as pl
from jax.experimental.pallas import tpu as pltpu
from jax.sharding import PartitionSpec as P

MESH = pl.DeviceIdType.MESH
BK = 512
VLIM = 60
DEAL = 3
RELAY = 4
RING = 6
CH = 4
SUB = 4
NH = 8


def _vmem():
    return pl.BlockSpec(memory_space=pltpu.VMEM)


def _hbm():
    return pl.BlockSpec(memory_space=pltpu.HBM)


def _smem():
    return pl.BlockSpec(memory_space=pltpu.SMEM)


def _qa_kernel(ne, nm, scale, lens, x, wq, wk, wv, kc, vc, ob, olast, k_out, v_out,
               xv, wqv, wkv, qsend, qrecv, qown, qc, qin, qa, qb, oa, obh, ost, knf, vnf, kbuf, vbuf,
               sa, sb, ma, mb, na, nb_,
               xsem, wsem, kvsem, ss0, sr0, ss, sr, hs, hr, osend, orecv, vsend, vrecv, ksem, vsem):
    i = lax.axis_index("emb")
    j = lax.axis_index("model")
    ie = 1 - i
    de = wq.shape[0]
    be = xv.shape[1] // 2
    bl = be // nm
    rows = bl // CH
    kk = wq.shape[1]
    cw = kk // NH
    dh = wk.shape[1]
    nh = ost.shape[2] // dh
    slots = kc.shape[1]
    start = i * be + j * bl

    def at(a, b):
        return {"emb": a, "model": b}

    def xcopy(a, r):
        row = pl.multiple_of((ie if a == 0 else i) * be, be)
        col = pl.multiple_of((i if r == 0 else ie) * de, de)
        return pltpu.make_async_copy(x.at[pl.ds(row, be), pl.ds(col, de)], xv.at[r, a * be:(a + 1) * be, :], xsem.at[a, r])

    def wcopy(h):
        return pltpu.make_async_copy(wq.at[:, pl.ds(h * cw, cw)], wqv.at[h], wsem.at[h])

    def kvcopy(n, r):
        src = wk if n == 0 else wv
        row = pl.multiple_of((i if r == 0 else ie) * de, de)
        return pltpu.make_async_copy(src.at[pl.ds(row, de), :], wkv.at[n, r], kvsem.at[n, r])

    def kcopy(n):
        slot = lax.rem(n, RING)
        return pltpu.make_async_copy(kc.at[start + n], kbuf.at[slot], ksem.at[slot])

    def vcopy(n):
        slot = lax.rem(n, RING)
        return pltpu.make_async_copy(vc.at[start + n], vbuf.at[slot], vsem.at[slot])

    xcopy(0, 0).start()
    for h in range(NH):
        wcopy(h).start()
    xcopy(1, 0).start()
    xcopy(0, 1).start()
    xcopy(1, 1).start()
    for n in range(2):
        for r in range(2):
            kvcopy(n, r).start()
    for n in range(RING - 1):
        kcopy(n).start()
        if n < RING - 2:
            vcopy(n).start()

    barrier = pltpu.get_barrier_semaphore()
    pl.semaphore_signal(barrier, inc=1, device_id=at(ie, j), device_id_type=MESH)
    for r in range(1, nm):
        pl.semaphore_signal(barrier, inc=1, device_id=at(i, lax.rem(j + r, nm)), device_id_type=MESH)
    pl.semaphore_wait(barrier, nm)

    def first(h):
        return pltpu.make_async_remote_copy(
            src_ref=qsend.at[0, :, pl.ds(h * cw, cw)], dst_ref=qrecv.at[0, :, pl.ds(h * cw, cw)],
            send_sem=ss0.at[h], recv_sem=sr0.at[h], device_id=at(ie, j), device_id_type=MESH)

    def later(s):
        return pltpu.make_async_remote_copy(
            src_ref=qsend.at[s], dst_ref=qrecv.at[s], send_sem=ss.at[s], recv_sem=sr.at[s],
            device_id=at(ie, j), device_id_type=MESH)

    def mycols(d):
        return pl.ds(pl.multiple_of(d * kk, kk), kk)

    def hcopy(s, r):
        d = lax.rem(j + r, nm)
        return pltpu.make_async_remote_copy(
            src_ref=qc.at[s, pl.ds(pl.multiple_of(d * rows, rows), rows), :], dst_ref=qin.at[s, :, mycols(j)],
            send_sem=hs.at[s, r], recv_sem=hr.at[s, nm - r], device_id=at(i, d), device_id_type=MESH)

    def hrecv(s, r):
        d = lax.rem(j + r, nm)
        return pltpu.make_async_remote_copy(
            src_ref=qc.at[s, pl.ds(0, rows), :], dst_ref=qin.at[s, :, mycols(d)],
            send_sem=hs.at[s, r], recv_sem=hr.at[s, r], device_id=at(i, d), device_id_type=MESH)

    def block(a, d):
        return pl.ds(pl.multiple_of((a * nm + d) * rows, rows), rows)

    def ocopy(s, r):
        d = lax.rem(j + r, nm)
        return pltpu.make_async_remote_copy(
            src_ref=ost.at[s, :, mycols(d)], dst_ref=ob.at[s, block(i, j), :],
            send_sem=osend.at[s, r], recv_sem=orecv.at[s, nm - r], device_id=at(i, d), device_id_type=MESH)

    def orecv_copy(s, r):
        d = lax.rem(j + r, nm)
        return pltpu.make_async_remote_copy(
            src_ref=ob.at[s, block(i, d), :], dst_ref=ob.at[s, block(i, d), :],
            send_sem=osend.at[s, r], recv_sem=orecv.at[s, r], device_id=at(i, d), device_id_type=MESH)

    def ycopy(s, r):
        dst = ob.at[s, block(i, lax.rem(j + r, nm)), :]
        return pltpu.make_async_remote_copy(
            src_ref=ost.at[s, :, mycols(j)] if r == 0 else dst, dst_ref=dst,
            send_sem=vsend.at[s, r], recv_sem=vrecv.at[s, r], device_id=at(ie, j), device_id_type=MESH)

    def yrecv_copy(s, r):
        blk = ob.at[s, block(ie, lax.rem(j + r, nm)), :]
        return pltpu.make_async_remote_copy(
            src_ref=blk, dst_ref=blk, send_sem=vsend.at[s, r], recv_sem=vrecv.at[s, r],
            device_id=at(ie, j), device_id_type=MESH)

    def spread(dst, h, val):
        for s in range(CH):
            for d in range(nm):
                dst[s, d * rows:(d + 1) * rows, h * cw:(h + 1) * cw] = val[d * bl + s * rows:d * bl + (s + 1) * rows]

    xcopy(0, 0).wait()
    for h in range(NH):
        wcopy(h).wait()
        spread(qsend, h, jnp.dot(xv[0, :be, :], wqv[h], preferred_element_type=jnp.float32))
        first(h).start()
    for s in range(1, CH):
        later(s).start()
    xcopy(1, 0).wait()
    for h in range(NH):
        spread(qown, h, jnp.dot(xv[0, be:, :], wqv[h], preferred_element_type=jnp.float32))
    def deal(s):
        qc[s] = (qown[s] + qrecv[s]).astype(jnp.bfloat16)
        for r in (2, 3, 1):
            hcopy(s, r).start()
        qin[s, :, mycols(j)] = qc[s, pl.ds(pl.multiple_of(j * rows, rows), rows), :]

    def relay(s):
        for r in range(1, nm):
            orecv_copy(s, r).wait_recv()
            ycopy(s, r).start()

    for h in range(NH):
        first(h).wait_recv()
    deal(0)

    xcopy(0, 1).wait()
    xcopy(1, 1).wait()
    for n in range(2):
        for r in range(2):
            kvcopy(n, r).wait()
    for n, out, rowf in ((0, k_out, knf), (1, v_out, vnf)):
        for a in range(2):
            acc = jnp.dot(xv[0, a * be:(a + 1) * be, :], wkv[n, 0], preferred_element_type=jnp.float32)
            acc += jnp.dot(xv[1, a * be:(a + 1) * be, :], wkv[n, 1], preferred_element_type=jnp.float32)
            out[pl.ds(pl.multiple_of((ie if a == 0 else i) * be, be), be), :] = acc.astype(jnp.bfloat16)
        rowf[...] = out[pl.ds(pl.multiple_of(start, bl), bl), :].astype(jnp.float32)

    def scores(n, sref, mref, nref):
        t = n % rows
        seq = pl.ds(pl.multiple_of(t * nh, nh), nh)
        qf = jnp.concatenate([qa[seq, :], qb[seq, :]], 1)
        q = qf.astype(jnp.bfloat16)
        slot = lax.rem(n, RING)
        new = jnp.sum(qf * knf[pl.ds(n, 1), :], axis=1, keepdims=True) * scale
        count = lens[start + n]
        top = None
        for b in range(slots // BK):
            v = lax.dot_general(q, kbuf[slot, b * BK:(b + 1) * BK, :], (((1,), (1,)), ((), ())),
                                preferred_element_type=jnp.float32) * scale
            v = jnp.where(lax.broadcasted_iota(jnp.int32, v.shape, 1) + b * BK < count, v, -jnp.inf)
            sref[:, b * BK:(b + 1) * BK] = v
            top = v if top is None else jnp.maximum(top, v)
        m = jnp.maximum(jnp.max(top, axis=1, keepdims=True), new)
        mref[...] = jnp.broadcast_to(m, mref.shape)
        nref[...] = jnp.broadcast_to(new, nref.shape)

    def values(n, sref, mref, nref):
        t = n % rows
        seq = pl.ds(pl.multiple_of(t * nh, nh), nh)
        slot = lax.rem(n, RING)
        m = mref[...]
        wide = jnp.concatenate([m] * (BK // 128), 1)
        ps, tot = [], None
        for b in range(slots // BK):
            p = jnp.exp(sref[:, b * BK:(b + 1) * BK] - wide)
            tot = p if tot is None else tot + p
            ps.append(p.astype(jnp.bfloat16))
        acc = jnp.dot(jnp.concatenate(ps, 1), vbuf[slot], preferred_element_type=jnp.float32)
        pn = jnp.exp(nref[...] - m)
        inv = 1.0 / (jnp.sum(tot, axis=1, keepdims=True) + pn)
        pn = pn.astype(jnp.bfloat16).astype(jnp.float32)
        vn = vnf[pl.ds(n, 1), :]
        oa[seq, :] = (acc[:, :128] + pn * vn[:, :128]) * inv
        obh[seq, :] = (acc[:, 128:] + pn * vn[:, 128:]) * inv

    A, B = (sa, ma, na), (sb, mb, nb_)

    def fetch(n):
        @pl.when(n + RING - 1 < bl)
        def _():
            kcopy(n + RING - 1).start()
            vcopy(n + RING - 2).start()

        @pl.when(n + RING - 1 == bl)
        def _():
            vcopy(n + RING - 2).start()

        @pl.when(n + RING < bl)
        def _():
            kcopy(n + RING).start()
            vcopy(n + RING - 1).start()

        @pl.when(n + RING == bl)
        def _():
            vcopy(n + RING - 1).start()

    per = rows // 2

    def load_q(s):
        for r in range(1, nm):
            hrecv(s, r).wait_recv()
        for h in range(nh):
            qa[pl.ds(h, rows, stride=nh), :] = qin[s, :, h * dh:h * dh + 128].astype(jnp.float32)
            qb[pl.ds(h, rows, stride=nh), :] = qin[s, :, h * dh + 128:(h + 1) * dh].astype(jnp.float32)

    def store_o(s):
        for h in range(nh):
            ost[s, :, h * dh:h * dh + 128] = oa[pl.ds(h, rows, stride=nh), :].astype(jnp.bfloat16)
            ost[s, :, h * dh + 128:(h + 1) * dh] = obh[pl.ds(h, rows, stride=nh), :].astype(jnp.bfloat16)

    load_q(0)
    kcopy(0).wait()
    scores(0, *A)

    def pair(p, c):
        n = 2 * p
        s = p // per
        t = p % per

        @pl.when(t == DEAL)
        def _():
            @pl.when(s + 1 < CH)
            def _():
                later(s + 1).wait_recv()
                deal(s + 1)

        @pl.when(t == RELAY)
        def _():
            @pl.when(s >= 1)
            def _():
                relay(s - 1)

        fetch(n)
        kcopy(n + 1).wait()
        vcopy(n).wait()
        values(n, *A)
        scores(n + 1, *B)

        @pl.when(t == per - 1)
        def _():
            load_q(s + 1)

        kcopy(n + 2).wait()
        vcopy(n + 1).wait()
        values(n + 1, *B)
        scores(n + 2, *A)

        @pl.when(t == per - 1)
        def _():
            store_o(s)
            for r in (2, 3, 1):
                ocopy(s, r).start()
            ycopy(s, 0).start()
            ob[s, block(i, j), :] = ost[s, :, mycols(j)]

        return c

    lax.fori_loop(0, bl // 2 - 1, pair, 0)
    kcopy(bl - 1).wait()
    vcopy(bl - 2).wait()
    values(bl - 2, *A)
    scores(bl - 1, *B)
    vcopy(bl - 1).wait()
    values(bl - 1, *B)
    store_o(CH - 1)
    olast[...] = ost[CH - 1]
    for h in range(NH):
        first(h).wait_send()
    for s in range(CH):
        if s:
            later(s).wait_send()
        for r in range(1, nm):
            hcopy(s, r).wait_send()
            if s < CH - 1:
                ocopy(s, r).wait_send()
        if s < CH - 1:
            for r in range(nm):
                ycopy(s, r).wait_send()
                yrecv_copy(s, r).wait_recv()


def _attend(x, Wq, Wk, Wv, Kc, Vc, lengths, ne, nm):
    b, d = x.shape
    de, kk = Wq.shape
    dh = Wk.shape[1]
    slots = Kc.shape[1]
    be = b // ne
    bl = be // nm
    rows = bl // CH
    cw = kk // NH
    full = kk * nm
    nh = full // dh
    assert dh == 256 and slots % BK == 0
    bf, f32 = jnp.bfloat16, jnp.float32
    dma = pltpu.SemaphoreType.DMA
    V = pltpu.VMEM
    part = V((CH, nm * rows, kk), f32)
    flat = V((rows * nh, 128), f32)
    stat = V((nh, 128), f32)
    return pl.pallas_call(
        functools.partial(_qa_kernel, ne, nm, dh ** -0.5),
        out_shape=(V((CH - 1, b // CH, kk), bf), V((rows, full), bf), V((b, dh), bf), V((b, dh), bf)),
        in_specs=[_smem()] + [_hbm()] * 6,
        out_specs=(_vmem(),) * 4,
        scratch_shapes=[
            V((2, b, de), bf), V((NH, de, cw), bf), V((2, 2, de, dh), bf), part, part, part,
            V((CH, nm * rows, kk), bf), V((CH, rows, full), bf), flat, flat, flat, flat, V((CH, rows, full), bf),
            V((bl, dh), f32), V((bl, dh), f32), V((RING, slots, dh), bf), V((RING, slots, dh), bf),
            V((nh, slots), f32), V((nh, slots), f32), stat, stat, stat, stat,
            dma((2, 2)), dma((NH,)), dma((2, 2)), dma((NH,)), dma((NH,)), dma((CH,)), dma((CH,)),
            dma((CH, nm)), dma((CH, nm)), dma((CH, nm)), dma((CH, nm)), dma((CH, nm)), dma((CH, nm)),
            dma((RING,)), dma((RING,)),
        ],
        compiler_params=pltpu.CompilerParams(collective_id=0, has_side_effects=True, vmem_limit_bytes=VLIM << 20),
        name="attend",
    )(lengths, x, Wq, Wk, Wv, Kc, Vc)


def _out_kernel(ne, nm, od_ref, o_ref, wo, x, y, wv, xv, ob, pown, psend, precv, ssend, srecv,
                wsem, xsem, osend, orecv, vsend, vrecv, ps, pr, xs_, xr, cs, cr, es, er, fs, fr):
    i = lax.axis_index("emb")
    j = lax.axis_index("model")
    c = lax.rem(j, 2)
    jp = j + 1 - 2 * c
    jx = lax.rem(j + 2, nm)
    ie = 1 - i
    half = wv.shape[2]
    cw = half // SUB
    rows = o_ref.shape[0]
    kk = wv.shape[1]
    dev = ne * nm

    def at(a, b):
        return {"emb": a, "model": b}

    def wcopy(b, u):
        col = pl.multiple_of((1 - c if b == 0 else c) * half + u * cw, cw)
        return pltpu.make_async_copy(wo.at[:, pl.ds(col, cw)], wv.at[b, :, pl.ds(u * cw, cw)], wsem.at[b, u])

    for b in range(2):
        for u in range(SUB):
            wcopy(b, u).start()
    mycol = pl.multiple_of((i * 2 + c) * half, half)
    excol = pl.multiple_of((ie * 2 + c) * half, half)
    xcopy = pltpu.make_async_copy(x.at[:, :, pl.ds(mycol, half)], xv, xsem)
    xcopy.start()

    barrier = pltpu.get_barrier_semaphore()
    pl.semaphore_signal(barrier, inc=1, device_id=at(ie, j), device_id_type=MESH)
    for r in range(1, nm):
        pl.semaphore_signal(barrier, inc=1, device_id=at(i, lax.rem(j + r, nm)), device_id_type=MESH)
    pl.semaphore_wait(barrier, nm)

    def block(a, d):
        return pl.ds(pl.multiple_of((a * nm + d) * rows, rows), rows)

    def heads(d):
        return pl.ds(pl.multiple_of(d * kk, kk), kk)

    def ocopy(r):
        d = lax.rem(j + r, nm)
        return pltpu.make_async_remote_copy(
            src_ref=o_ref.at[:, heads(d)], dst_ref=ob.at[block(i, j), :],
            send_sem=osend.at[r], recv_sem=orecv.at[nm - r], device_id=at(i, d), device_id_type=MESH)

    def orecv_copy(r):
        d = lax.rem(j + r, nm)
        return pltpu.make_async_remote_copy(
            src_ref=ob.at[block(i, d), :], dst_ref=ob.at[block(i, d), :],
            send_sem=osend.at[r], recv_sem=orecv.at[r], device_id=at(i, d), device_id_type=MESH)

    def vcopy(r):
        dst = ob.at[block(i, lax.rem(j + r, nm)), :]
        return pltpu.make_async_remote_copy(
            src_ref=o_ref.at[:, heads(j)] if r == 0 else dst, dst_ref=dst,
            send_sem=vsend.at[r], recv_sem=vrecv.at[r], device_id=at(ie, j), device_id_type=MESH)

    def vrecv_copy(r):
        blk = ob.at[block(ie, lax.rem(j + r, nm)), :]
        return pltpu.make_async_remote_copy(
            src_ref=blk, dst_ref=blk, send_sem=vsend.at[r], recv_sem=vrecv.at[r],
            device_id=at(ie, j), device_id_type=MESH)

    for r in (2, 3, 1):
        ocopy(r).start()
    vcopy(0).start()
    ob[block(i, j), :] = o_ref[:, heads(j)]

    def pcopy(s, u):
        return pltpu.make_async_remote_copy(
            src_ref=psend.at[s, u], dst_ref=precv.at[s, u], send_sem=ps.at[s, u], recv_sem=pr.at[s, u],
            device_id=at(i, jp), device_id_type=MESH)

    def scopy(s, u):
        return pltpu.make_async_remote_copy(
            src_ref=ssend.at[s, u], dst_ref=srecv.at[s, u], send_sem=xs_.at[s, u], recv_sem=xr.at[s, u],
            device_id=at(i, jx), device_id_type=MESH)

    def piece(s, u, base):
        return y.at[:, pl.ds(pl.multiple_of(s * rows, rows), rows), pl.ds(pl.multiple_of(base + u * cw, cw), cw)]

    def ccopy(s, u):
        return pltpu.make_async_remote_copy(
            src_ref=piece(s, u, mycol), dst_ref=piece(s, u, mycol), send_sem=cs.at[s, u], recv_sem=cr.at[s, u],
            device_id=at(i, jp), device_id_type=MESH)

    def ecopy(s, u):
        return pltpu.make_async_remote_copy(
            src_ref=piece(s, u, mycol), dst_ref=piece(s, u, mycol), send_sem=es.at[s, u], recv_sem=er.at[s, u],
            device_id=at(ie, j), device_id_type=MESH)

    def fcopy(s, u):
        return pltpu.make_async_remote_copy(
            src_ref=piece(s, u, excol), dst_ref=piece(s, u, excol), send_sem=fs.at[s, u], recv_sem=fr.at[s, u],
            device_id=at(i, jp), device_id_type=MESH)

    def compute(s, lhs):
        for u in range(SUB):
            @pl.when(s == 0)
            def _():
                wcopy(0, u).wait()

            psend[s, u] = jnp.dot(lhs(), wv[0, :, u * cw:(u + 1) * cw],
                                  preferred_element_type=jnp.float32).astype(jnp.bfloat16)
            pcopy(s, u).start()
        for u in range(SUB):
            @pl.when(s == 0)
            def _():
                wcopy(1, u).wait()

            pown[u] = jnp.dot(lhs(), wv[1, :, u * cw:(u + 1) * cw], preferred_element_type=jnp.float32)
            pcopy(s, u).wait_recv()
            ssend[s, u] = (pown[u] + precv[s, u].astype(jnp.float32)).astype(jnp.bfloat16)
            scopy(s, u).start()

    def finish(s):
        at_rows = pl.ds(pl.multiple_of(s * rows, rows), rows)
        for u in range(SUB):
            scopy(s, u).wait_recv()
            tot = ssend[s, u].astype(jnp.float32) + srecv[s, u].astype(jnp.float32)
            xs = xv[:, at_rows, u * cw:(u + 1) * cw].astype(jnp.float32)
            y[:, at_rows, pl.ds(pl.multiple_of(mycol + u * cw, cw), cw)] = (
                xs + tot.reshape(dev, rows, cw)).astype(jnp.bfloat16)
            ecopy(s, u).start()
            ccopy(s, u).start()

    def forward(s):
        for u in range(SUB):
            ecopy(s, u).wait_recv()
            fcopy(s, u).start()

    def step(s, carry):
        compute(s, lambda: od_ref[s])

        @pl.when(s == 0)
        def _():
            for r in range(1, nm):
                orecv_copy(r).wait_recv()
                vcopy(r).start()
            xcopy.wait()

        @pl.when(s >= 1)
        def _():
            finish(s - 1)

        @pl.when(s >= 2)
        def _():
            forward(s - 2)

        return carry

    lax.fori_loop(0, CH - 1, step, 0)
    for r in range(nm):
        vrecv_copy(r).wait_recv()
    compute(CH - 1, lambda: ob[...])
    finish(CH - 2)
    forward(CH - 3)
    finish(CH - 1)
    forward(CH - 2)
    forward(CH - 1)
    for r in range(1, nm):
        ocopy(r).wait_send()
    for r in range(nm):
        vcopy(r).wait_send()
    for s in range(CH):
        for u in range(SUB):
            pcopy(s, u).wait_send()
            scopy(s, u).wait_send()
            ecopy(s, u).wait_send()
            ccopy(s, u).wait()
            fcopy(s, u).wait()


def _project_out(done, last, Wo, x, ne, nm):
    bl = CH * last.shape[0]
    kk, ncol = Wo.shape
    half = ncol // 2
    dev = ne * nm
    rows = bl // CH
    cw = half // SUB
    b, d = x.shape
    bf, f32 = jnp.bfloat16, jnp.float32
    dma = pltpu.SemaphoreType.DMA
    pieces = pltpu.VMEM((CH, SUB, dev * rows, cw), bf)
    y = pl.pallas_call(
        functools.partial(_out_kernel, ne, nm),
        out_shape=pltpu.VMEM((dev, bl, d), bf),
        in_specs=[_vmem(), _vmem(), _hbm(), _hbm()],
        out_specs=_vmem(),
        scratch_shapes=[
            pltpu.VMEM((2, kk, half), bf), pltpu.VMEM((dev, bl, half), bf), pltpu.VMEM((dev * rows, kk), bf),
            pltpu.VMEM((SUB, dev * rows, cw), f32), pieces, pieces, pieces, pieces,
            dma((2, SUB)), dma,
        ] + [dma((nm,))] * 4 + [dma((CH, SUB))] * 10,
        compiler_params=pltpu.CompilerParams(collective_id=1, has_side_effects=True, vmem_limit_bytes=48 << 20),
        name="project_out",
    )(*[pltpu.with_memory_space_constraint(a, pltpu.VMEM) for a in (done, last)], Wo, x.reshape(dev, bl, d))
    return y.reshape(b, d)


def _write_kernel(y, k, v, yo, ko, vo, sem):
    copies = [pltpu.make_async_copy(a, b, sem.at[n]) for n, (a, b) in enumerate(((y, yo), (k, ko), (v, vo)))]
    for c in copies:
        c.start()
    for c in copies:
        c.wait()


def _write(y, k, v):
    return pl.pallas_call(
        _write_kernel,
        out_shape=tuple(jax.ShapeDtypeStruct(a.shape, a.dtype) for a in (y, k, v)),
        in_specs=[_vmem()] * 3,
        out_specs=(_hbm(),) * 3,
        scratch_shapes=[pltpu.SemaphoreType.DMA((3,))],
        compiler_params=pltpu.CompilerParams(vmem_limit_bytes=16 << 20),
        name="write",
    )(y, k, v)


def solution(mesh):
    ne = mesh.shape['emb']
    nm = mesh.shape['model']

    def local(x, Wq, Wk, Wv, Wo, Kc, Vc, lengths):
        done, last, k_new, v_new = _attend(x, Wq, Wk, Wv, Kc, Vc, lengths, ne, nm)
        y = _project_out(done, last, Wo, x, ne, nm)
        return _write(y, k_new, v_new)

    in_specs = (P('rep', None), P('emb', 'model'), P(), P(), P('model', 'emb'),
                P('rep', None, None), P('rep', None, None), P('rep'))
    out_specs = (P('rep', None), P('rep', None), P('rep', None))
    return jax.shard_map(local, mesh=mesh, in_specs=in_specs, out_specs=out_specs, check_vma=False)
```
